8 devices in a mesh: dp: 1 (over z), y: 2 (over y), x: 4 (over x, core).
Axes of the slice: x: 2, y: 2, z: 1, core: 2. Of those that a mesh axis runs over, the one named last changes fastest.
Arguments:
- tokens: int32 [3, 256], P(None, 'dp')
- lengths: int32 [256], P('dp')
- choices: int32 [3, 256, 8], P(None, 'dp')
- emb_table: bfloat16 [49155, 1536], P(None, 'x')
- k_cache: bfloat16 [256, 256, 8, 64], P('dp', None, 'y')
- v_cache: bfloat16 [256, 256, 8, 64], P('dp', None, 'y')
- g_attn: bfloat16 [1536], P('x')
- w_q: bfloat16 [1536, 1536], P('x', 'y')
- w_k: bfloat16 [1536, 512], P('x', 'y')
- w_v: bfloat16 [1536, 512], P('x', 'y')
- w_o: bfloat16 [1536, 1536], P('y', 'x')
- g_ffn: bfloat16 [1536], P('x')
- w_router: bfloat16 [1536, 40], P('x')
- w_act: bfloat16 [40, 1536, 512], P(None, 'x', 'y')
- w_lin: bfloat16 [40, 1536, 512], P(None, 'x', 'y')
- w_down: bfloat16 [40, 512, 1536], P(None, 'y', 'x')
Outputs:
- output 1: bfloat16 [3, 256, 1536], P(None, 'dp', 'x')
- output 2: bfloat16 [256, 256, 8, 64], P('dp', None, 'y')
- output 3: bfloat16 [256, 256, 8, 64], P('dp', None, 'y')
All inputs are finite; a program needn't handle non-finite values.
Results may differ from the reference program's by a relative error of at most 0.0112615.
Values are sent between devices in bfloat16 or wider.
A program may use at most 1 GiB of HBM per device.

```python
import math
import jax
import jax.numpy as jnp
from jax import lax

BATCH = 256
SEQ = 256
D = 1536
HEADS = 24
KV_HEADS = 8
HEAD = 64
FF = 512
EXPERTS = 40
TOP = 8
VOCAB = 49155
STEPS = 3

EPS = 1e-5
ROPE_BASE = 1.0e6
LOG_SEQ = int(math.log2(SEQ))
HOT_COUNT = max(1, EXPERTS // 8)
GROUP_SIZE = HEADS // KV_HEADS


def draw_lengths(key_a, key_b, key_c):
    exponent = jax.random.randint(key_a, (BATCH,), 0, LOG_SEQ + 1)
    len_limit = jnp.minimum(jnp.left_shift(jnp.ones((BATCH,), jnp.int32), exponent), SEQ - 3)
    raw_draw = jax.random.randint(key_b, (BATCH,), 0, 1 << 30)
    lengths = 1 + raw_draw % len_limit
    pick_row = jax.random.randint(key_c, (), 0, BATCH)
    row_ids = jnp.arange(BATCH)
    lengths = jnp.where(row_ids == pick_row, SEQ - 3, lengths)
    lengths = jnp.where(row_ids == (pick_row + 1) % BATCH, 1, lengths)
    return lengths.astype(jnp.int32)


def draw_choices(key_a, key_b):
    expert_rank = jax.random.permutation(key_a, EXPERTS)
    hot_bonus = jnp.where(expert_rank < HOT_COUNT, EXPERTS, 0)
    noise_int = jax.random.randint(key_b, (STEPS, BATCH, EXPERTS), 0, 2 * EXPERTS)
    scores = (noise_int + hot_bonus) * EXPERTS + jnp.arange(EXPERTS)
    return lax.top_k(scores, TOP)[1].astype(jnp.int32)


def normal_weights(key_w, shape_w, scale_w):
    return (jax.random.normal(key_w, shape_w, jnp.float32) * scale_w).astype(jnp.bfloat16)


def setup_inputs(seed: int = 0, part: int = 0) -> dict:
    base_key = jax.random.key(seed)
    weight_keys = jax.random.split(base_key, 12)
    part_keys = jax.random.split(jax.random.fold_in(base_key, part), 8)
    tokens = jax.random.randint(part_keys[0], (STEPS, BATCH), 0, VOCAB)
    lengths = draw_lengths(part_keys[1], part_keys[2], part_keys[3])
    choices = draw_choices(part_keys[4], part_keys[5])
    k_cache = normal_weights(part_keys[6], (BATCH, SEQ, KV_HEADS, HEAD), 1.0)
    v_cache = normal_weights(part_keys[7], (BATCH, SEQ, KV_HEADS, HEAD), 1.0)
    ramp_rate = jax.random.uniform(weight_keys[0], (), jnp.float32, 0.6, 1.2)
    col_scale = jnp.exp(ramp_rate * jnp.linspace(-1.0, 1.0, D))
    emb_table = (jax.random.normal(weight_keys[1], (VOCAB, D), jnp.float32) * col_scale).astype(jnp.bfloat16)
    g_attn = (1.0 + 0.3 * jax.random.normal(weight_keys[2], (D,), jnp.float32)).astype(jnp.bfloat16)
    w_q = normal_weights(weight_keys[3], (D, HEADS * HEAD), D ** -0.5)
    w_k = normal_weights(weight_keys[4], (D, KV_HEADS * HEAD), D ** -0.5)
    w_v = normal_weights(weight_keys[5], (D, KV_HEADS * HEAD), D ** -0.5)
    w_o = normal_weights(weight_keys[6], (HEADS * HEAD, D), (HEADS * HEAD) ** -0.5)
    g_ffn = (1.0 + 0.3 * jax.random.normal(weight_keys[7], (D,), jnp.float32)).astype(jnp.bfloat16)
    w_router = normal_weights(weight_keys[8], (D, EXPERTS), 1.5 * D ** -0.5)
    w_act = normal_weights(weight_keys[9], (EXPERTS, D, FF), D ** -0.5)
    w_lin = normal_weights(weight_keys[10], (EXPERTS, D, FF), D ** -0.5)
    w_down = normal_weights(weight_keys[11], (EXPERTS, FF, D), FF ** -0.5)
    return dict(tokens=tokens, lengths=lengths, choices=choices, emb_table=emb_table, k_cache=k_cache, v_cache=v_cache, g_attn=g_attn, w_q=w_q, w_k=w_k, w_v=w_v, w_o=w_o, g_ffn=g_ffn, w_router=w_router, w_act=w_act, w_lin=w_lin, w_down=w_down)


def rms_norm(x_val, gain_vec):
    x_f32 = x_val.astype(jnp.float32)
    meansq = jnp.sum(x_f32 * x_f32, axis=-1, keepdims=True) / D
    return (x_f32 * lax.rsqrt(meansq + EPS) * gain_vec.astype(jnp.float32)).astype(jnp.bfloat16)


def rotate(vectors, positions):
    half_dim = HEAD // 2
    inv_freq = ROPE_BASE ** (-(jnp.arange(half_dim).astype(jnp.float32) * 2.0 / HEAD))
    angles = positions.astype(jnp.float32)[:, None, None] * inv_freq
    cosine = jnp.cos(angles)
    sine_val = jnp.sin(angles)
    first_half = vectors[..., :half_dim].astype(jnp.float32)
    second_half = vectors[..., half_dim:].astype(jnp.float32)
    return jnp.concatenate([first_half * cosine - second_half * sine_val, second_half * cosine + first_half * sine_val], axis=-1).astype(jnp.bfloat16)


def attend_row(row_args):
    q_row, key_row, val_row, pos_row = row_args
    scores = jnp.einsum('kgh,skh->kgs', q_row.astype(jnp.float32), key_row.astype(jnp.float32)) * HEAD ** -0.5
    valid_mask = jnp.arange(SEQ) <= pos_row
    scores = jnp.where(valid_mask, scores, -1.0e30)
    peak_val = jnp.max(scores, axis=-1, keepdims=True)
    weight = jnp.where(valid_mask, jnp.exp(scores - peak_val), 0.0)
    total_w = jnp.sum(weight, axis=-1, keepdims=True)
    mixed_out = jnp.einsum('kgs,skh->kgh', weight.astype(jnp.bfloat16).astype(jnp.float32), val_row.astype(jnp.float32))
    return (mixed_out / total_w).astype(jnp.bfloat16)


def reference(tokens, lengths, choices, emb_table, k_cache, v_cache, g_attn, w_q, w_k, w_v, w_o, g_ffn, w_router, w_act, w_lin, w_down):
    slot_ids = jnp.arange(SEQ)
    expert_ids = jnp.arange(EXPERTS)

    def one_step(carry, step_in):
        key_cache, val_cache = carry
        tok_row, choice_row, step_idx = step_in
        positions = lengths + step_idx
        x_in = emb_table[tok_row]
        normed = rms_norm(x_in, g_attn)
        queries = rotate(jnp.dot(normed, w_q, preferred_element_type=jnp.float32).astype(jnp.bfloat16).reshape(BATCH, HEADS, HEAD), positions)
        new_keys = rotate(jnp.dot(normed, w_k, preferred_element_type=jnp.float32).astype(jnp.bfloat16).reshape(BATCH, KV_HEADS, HEAD), positions)
        new_vals = jnp.dot(normed, w_v, preferred_element_type=jnp.float32).astype(jnp.bfloat16).reshape(BATCH, KV_HEADS, HEAD)
        hit_mask = (slot_ids[None, :] == positions[:, None])[:, :, None, None]
        key_cache = jnp.where(hit_mask, new_keys[:, None], key_cache)
        val_cache = jnp.where(hit_mask, new_vals[:, None], val_cache)
        grouped = queries.reshape(BATCH, KV_HEADS, GROUP_SIZE, HEAD)
        mixed = lax.map(attend_row, (grouped, key_cache, val_cache, positions)).reshape(BATCH, HEADS * HEAD)
        x_mid = (x_in.astype(jnp.float32) + jnp.dot(mixed, w_o, preferred_element_type=jnp.float32)).astype(jnp.bfloat16)
        normed2 = rms_norm(x_mid, g_ffn)
        logits = jnp.dot(normed2, w_router, preferred_element_type=jnp.float32)
        gate_val = jax.nn.softmax(jnp.take_along_axis(logits, choice_row, axis=1), axis=-1)
        onehot = choice_row[:, :, None] == expert_ids[None, None, :]
        coef = jnp.sum(jnp.where(onehot, gate_val[:, :, None], 0.0), axis=1)

        def expert_out(expert_args):
            act_w, lin_w, down_w, coef_col = expert_args
            act_f32 = jnp.dot(normed2, act_w, preferred_element_type=jnp.float32)
            lin_f32 = jnp.dot(normed2, lin_w, preferred_element_type=jnp.float32)
            unit_bf16 = (coef_col[:, None] * jax.nn.silu(act_f32) * lin_f32).astype(jnp.bfloat16)
            return jnp.dot(unit_bf16, down_w, preferred_element_type=jnp.float32)

        moe_sum = jnp.sum(lax.map(expert_out, (w_act, w_lin, w_down, coef.T)), axis=0)
        hidden_out = (x_mid.astype(jnp.float32) + moe_sum).astype(jnp.bfloat16)
        return (key_cache, val_cache), hidden_out

    (k_out, v_out), hidden_out = lax.scan(one_step, (k_cache, v_cache), (tokens, choices, jnp.arange(STEPS)))
    return hidden_out, k_out, v_out
```

```python
import functools

import jax
import jax.numpy as jnp
from jax import lax
from jax.experimental import pallas as pl
from jax.experimental.pallas import tpu as pltpu
from jax.sharding import PartitionSpec as P

EPS = 1e-5
ROPE_BASE = 1.0e6
F32 = jnp.float32
BF16 = jnp.bfloat16
VMEM_LIMIT = 60 * 1024 * 1024
NCHUNK = 1
NB = 8


def vspec():
    return pl.BlockSpec(memory_space=pltpu.VMEM)


def qkv_kernel(me_ref, x0, x1, x2, x3, gain_ref, w0, w1, w2, w3, cos_ref, sin_ref, out_ref, hs, ws):
    tile = pl.program_id(0)
    me = me_ref[0]
    place = [me, me + 1 - 2 * (me % 2), (me + 2) % 4]
    place.append((place[1] + 2) % 4)

    @pl.when(tile == 0)
    def _():
        xs = [r[...].astype(F32) for r in (x0, x1, x2, x3)]
        sq = [jnp.sum(v * v, axis=-1, keepdims=True) for v in xs]
        total = (sq[0] + sq[1]) + (sq[2] + sq[3])
        scale = lax.rsqrt(total / (4.0 * x0.shape[1]) + EPS)
        for i, ref in enumerate((x0, x1, x2, x3)):
            hs[place[i]] = (ref[...].astype(F32) * scale * gain_ref[i : i + 1, :]).astype(BF16)

    for i, ref in enumerate((w0, w1, w2, w3)):
        ws[place[i]] = ref[0]
    acc = jnp.dot(hs[0], ws[0], preferred_element_type=F32)
    for i in range(1, 4):
        acc += jnp.dot(hs[i], ws[i], preferred_element_type=F32)
    vals = acc.astype(BF16)

    @pl.when(tile < 4)
    def _():
        v = vals.astype(F32)
        lane = lax.broadcasted_iota(jnp.int32, (1, 256), 1) % 64
        low = lane < 32
        ahead = jnp.concatenate([v[:, 32:], v[:, :32]], axis=1)
        behind = jnp.concatenate([v[:, 224:], v[:, :224]], axis=1)
        other = jnp.where(low, ahead, behind)
        cos = jnp.concatenate([cos_ref[...], cos_ref[...]], axis=1)
        sin = jnp.concatenate([sin_ref[...], sin_ref[...]], axis=1)
        out_ref[0] = (v * cos + other * sin).astype(BF16)

    @pl.when(tile == 4)
    def _():
        out_ref[0] = vals


def qkv_call(me, xs, gains, ws, cos, sin):
    tokens, width = xs[0].shape
    grid_spec = pltpu.PrefetchScalarGridSpec(
        num_scalar_prefetch=1,
        grid=(5,),
        in_specs=[pl.BlockSpec((tokens, width), lambda i, m: (0, 0))] * 4
        + [pl.BlockSpec((4, width), lambda i, m: (0, 0))]
        + [pl.BlockSpec((1, width, 256), lambda i, m: (i, 0, 0))] * 4
        + [pl.BlockSpec((tokens, 128), lambda i, m: (0, 0))] * 2,
        out_specs=pl.BlockSpec((1, tokens, 256), lambda i, m: (i, 0, 0)),
        scratch_shapes=[pltpu.VMEM((4, tokens, width), BF16), pltpu.VMEM((4, width, 256), BF16)],
    )
    return pl.pallas_call(
        qkv_kernel,
        grid_spec=grid_spec,
        out_shape=jax.ShapeDtypeStruct((5, tokens, 256), BF16),
        compiler_params=pltpu.CompilerParams(vmem_limit_bytes=VMEM_LIMIT, dimension_semantics=("arbitrary",)),
        cost_estimate=pl.CostEstimate(flops=2 * tokens * width * 4 * 1280, bytes_accessed=9_000_000, transcendentals=0),
        name="qkv",
    )(me, *xs, gains, *ws, cos, sin)


def attn_kernel(len_ref, a_ref, k_ref, v_ref, o_ref, ko_ref, vo_ref):
    step = pl.program_id(0)
    nb = a_ref.shape[0]
    cols = jnp.transpose(a_ref[...].reshape(nb * 16, 256).astype(F32))
    slot = lax.broadcasted_iota(jnp.int32, (1, 256), 1)
    block = lax.broadcasted_iota(jnp.int32, (1, 256), 1) // 64
    row_t = lax.broadcasted_iota(jnp.int32, (64, 1), 0) % 16 % 3
    for i in range(nb):
        pos = len_ref[step * nb + i]
        kt = k_ref[i * 256 : (i + 1) * 256, :]
        vt = v_ref[i * 256 : (i + 1) * 256, :]
        for t in range(3):
            hit = slot == pos + t
            c0 = i * 16 + 9 + t
            kt = jnp.where(hit, cols[:, c0 : c0 + 1].astype(BF16), kt)
            vt = jnp.where(hit, cols[:, c0 + 3 : c0 + 4].astype(BF16), vt)
        ko_ref[i * 256 : (i + 1) * 256, :] = kt
        vo_ref[i * 256 : (i + 1) * 256, :] = vt
        q = a_ref[i]
        zero = jnp.zeros_like(q)
        lhs = jnp.concatenate([jnp.where(block == k, q, zero) for k in range(4)], axis=0)
        s = jnp.dot(lhs, kt, preferred_element_type=F32) * 0.125
        valid = slot <= row_t + pos
        s = jnp.where(valid, s, -1.0e30)
        peak = jnp.max(s, axis=-1, keepdims=True)
        e = jnp.where(valid, jnp.exp(s - peak), 0.0)
        total = jnp.sum(e, axis=-1, keepdims=True)
        mixed = lax.dot_general(e.astype(BF16), vt, (((1,), (1,)), ((), ())), preferred_element_type=F32)
        mixed = mixed / total
        res = mixed[0:16]
        for k in range(1, 4):
            res = jnp.where(block == k, mixed[16 * k : 16 * k + 16], res)
        o_ref[i] = res.astype(BF16)


def attn_call(lengths, acts, k_rows, v_rows):
    batch = acts.shape[0]
    grid_spec = pltpu.PrefetchScalarGridSpec(
        num_scalar_prefetch=1,
        grid=(batch // NB,),
        in_specs=[pl.BlockSpec((NB, 16, 256), lambda i, m: (i, 0, 0))] + [pl.BlockSpec((NB * 256, 256), lambda i, m: (i, 0))] * 2,
        out_specs=[pl.BlockSpec((NB, 16, 256), lambda i, m: (i, 0, 0))] + [pl.BlockSpec((NB * 256, 256), lambda i, m: (i, 0))] * 2,
    )
    return pl.pallas_call(
        attn_kernel,
        grid_spec=grid_spec,
        out_shape=[
            jax.ShapeDtypeStruct((batch, 16, 256), BF16),
            jax.ShapeDtypeStruct(k_rows.shape, BF16),
            jax.ShapeDtypeStruct(v_rows.shape, BF16),
        ],
        compiler_params=pltpu.CompilerParams(vmem_limit_bytes=VMEM_LIMIT, dimension_semantics=("arbitrary",)),
        cost_estimate=pl.CostEstimate(flops=40_000_000_000, bytes_accessed=134_000_000, transcendentals=0),
        name="attn",
    )(lengths, acts, k_rows, v_rows)


E1 = 4


def moe1_kernel(cx_ref, h_ref, ch_ref, a0, l0, a1, l1, keep_ref, send_ref, dense):
    step = pl.program_id(0)
    half = keep_ref.shape[1]
    for k in range(E1):
        top = jnp.concatenate([a0[k], l0[k]], axis=1)
        low = jnp.concatenate([a1[k], l1[k]], axis=1)
        w = jnp.concatenate([top, low], axis=0)
        dense[k] = jnp.dot(h_ref[...], w, preferred_element_type=F32).astype(BF16)
    cx = cx_ref[0]
    rt = 32

    def run(first):
        for part, ref in ((0, keep_ref), (1, send_ref)):
            row0 = ((cx + part) % 2) * half

            def body(i, carry):
                src = pl.ds(pl.multiple_of(row0 + i * rt, rt), rt)
                dst = pl.ds(pl.multiple_of(i * rt, rt), rt)
                d = [dense[k, src, :] for k in range(E1)]
                for j in range(8):
                    chj = ch_ref[j, src, :]
                    hits = [chj == (step * E1 + k).astype(F32).astype(BF16) for k in range(E1)]
                    for side in range(2):
                        lanes = slice(side * 128, side * 128 + 128)
                        acc = jnp.zeros((rt, 128), BF16) if first else ref[j, dst, lanes]
                        for k in range(E1):
                            acc = jnp.where(hits[k], d[k][:, lanes], acc)
                        ref[j, dst, lanes] = acc
                return carry

            lax.fori_loop(0, half // rt, body, 0)

    @pl.when(step == 0)
    def _():
        run(True)

    @pl.when(step > 0)
    def _():
        run(False)


def moe1_call(cx, h2, ch, a0, l0, a1, l1):
    tokens = h2.shape[0]
    experts, rows, _ = a0.shape
    out = jax.ShapeDtypeStruct((8, tokens // 2, 256), BF16)
    grid_spec = pltpu.PrefetchScalarGridSpec(
        num_scalar_prefetch=1,
        grid=(experts // E1,),
        in_specs=[pl.BlockSpec((tokens, 2 * rows), lambda i, m: (0, 0)), pl.BlockSpec((8, tokens, 128), lambda i, m: (0, 0, 0))]
        + [pl.BlockSpec((E1, rows, 128), lambda i, m: (i, 0, 0))] * 4,
        out_specs=[pl.BlockSpec((8, tokens // 2, 256), lambda i, m: (0, 0, 0))] * 2,
        scratch_shapes=[pltpu.VMEM((E1, tokens, 256), BF16)],
    )
    return pl.pallas_call(
        moe1_kernel,
        grid_spec=grid_spec,
        out_shape=[out, out],
        compiler_params=pltpu.CompilerParams(vmem_limit_bytes=VMEM_LIMIT, dimension_semantics=("arbitrary",)),
        cost_estimate=pl.CostEstimate(flops=2 * tokens * 2 * rows * 256 * experts, bytes_accessed=20_000_000, transcendentals=0),
        name="moe1",
    )(cx, h2, ch, a0, l0, a1, l1)


E2 = 4


def moe2_kernel(cx_ref, um_ref, uo_ref, ch_ref, wa, wb, own_ref, send_ref, spread, acc_ref):
    step = pl.program_id(0)
    half = um_ref.shape[1]
    width = wa.shape[2]
    cx = cx_ref[0]
    rt = 32
    for part, ref in ((0, um_ref), (1, uo_ref)):
        row0 = ((cx + part) % 2) * half

        def body(i, carry):
            dst = pl.ds(pl.multiple_of(row0 + i * rt, rt), rt)
            src = pl.ds(pl.multiple_of(i * rt, rt), rt)
            out = [jnp.zeros((rt, 128), BF16) for _ in range(E2)]
            for j in range(8):
                chj = ch_ref[j, dst, :]
                uj = ref[j, src, :]
                for k in range(E2):
                    out[k] = jnp.where(chj == (step * E2 + k).astype(F32).astype(BF16), uj, out[k])
            for k in range(E2):
                spread[dst, k * 128 : (k + 1) * 128] = out[k]
            return carry

        lax.fori_loop(0, half // rt, body, 0)
    w = jnp.concatenate([wa[...].reshape(E2 * 128, width), wb[...].reshape(E2 * 128, width)], axis=1)
    prod = jnp.dot(spread[...], w, preferred_element_type=F32)

    @pl.when(step == 0)
    def _():
        acc_ref[...] = prod

    @pl.when(step > 0)
    def _():
        acc_ref[...] += prod

    @pl.when(step == pl.num_programs(0) - 1)
    def _():
        own_ref[...] = acc_ref[:, :width]
        send_ref[...] = acc_ref[:, width:].astype(BF16)


def moe2_call(cx, um, uo, ch, wa, wb):
    tokens = ch.shape[1]
    experts, rows, width = wa.shape
    grid_spec = pltpu.PrefetchScalarGridSpec(
        num_scalar_prefetch=1,
        grid=(experts // E2,),
        in_specs=[pl.BlockSpec((8, tokens // 2, 128), lambda i, m: (0, 0, 0))] * 2
        + [pl.BlockSpec((8, tokens, 128), lambda i, m: (0, 0, 0))]
        + [pl.BlockSpec((E2, rows, width), lambda i, m: (i, 0, 0))] * 2,
        out_specs=[pl.BlockSpec((tokens, width), lambda i, m: (0, 0))] * 2,
        scratch_shapes=[pltpu.VMEM((tokens, E2 * 128), BF16), pltpu.VMEM((tokens, 2 * width), F32)],
    )
    return pl.pallas_call(
        moe2_kernel,
        grid_spec=grid_spec,
        out_shape=[jax.ShapeDtypeStruct((tokens, width), F32), jax.ShapeDtypeStruct((tokens, width), BF16)],
        compiler_params=pltpu.CompilerParams(vmem_limit_bytes=VMEM_LIMIT, dimension_semantics=("arbitrary",)),
        cost_estimate=pl.CostEstimate(flops=2 * tokens * rows * 2 * width * experts, bytes_accessed=10_000_000, transcendentals=0),
        name="moe2",
    )(cx, um, uo, ch, wa, wb)


def solution(mesh):
    cache_spec = P('dp', None, 'y', None)
    in_specs = (P(None, 'dp'), P('dp'), P(None, 'dp', None), P(None, 'x'), cache_spec, cache_spec, P('x'), P('x', 'y'), P('x', 'y'), P('x', 'y'), P('y', 'x'), P('x'), P('x', None), P(None, 'x', 'y'), P(None, 'x', 'y'), P(None, 'y', 'x'))
    out_specs = (P(None, 'dp', 'x'), cache_spec, cache_spec)

    def core_swap(v):
        return lax.ppermute(v, 'x', [(0, 1), (1, 0), (2, 3), (3, 2)])

    def chip_swap(v):
        return lax.ppermute(v, 'x', [(0, 2), (2, 0), (1, 3), (3, 1)])

    def y_swap(v):
        return lax.ppermute(v, 'y', [(0, 1), (1, 0)])

    def per_device(tokens, lengths, choices, emb_table, k_cache, v_cache, g_attn, w_q, w_k, w_v, w_o, g_ffn, w_router, w_act, w_lin, w_down):
        steps, batch = tokens.shape
        width = emb_table.shape[1]
        kv, hd = k_cache.shape[2], k_cache.shape[3]
        slots = k_cache.shape[1]
        group = w_q.shape[1] // (kv * hd)
        experts = w_act.shape[0]
        width_full = width * 4
        me = lax.axis_index('x').astype(jnp.int32)
        my = lax.axis_index('y').astype(jnp.int32)
        core = me % 2
        cx = me // 2
        n_tok = steps * batch

        wq = w_q.reshape(width, kv, group, hd).transpose(2, 0, 1, 3).reshape(group, width, kv * hd)
        w0 = jnp.concatenate([wq, w_k[None], w_v[None]], axis=0)
        w2 = chip_swap(w0)
        w1 = core_swap(w0)
        w3 = core_swap(w2)
        gains = jnp.stack([g_attn, g_ffn]).astype(F32)
        gains_c = core_swap(gains)
        gains_x = chip_swap(jnp.concatenate([gains, gains_c], axis=0))
        gain4 = jnp.stack([gains[0], gains_c[0], gains_x[0], gains_x[2]])

        x_in = jnp.take(emb_table, tokens.reshape(n_tok), axis=0, mode='clip')
        x_mate = core_swap(x_in)
        half_tok = n_tok // 2
        part = chip_swap(lax.dynamic_slice_in_dim(x_in, my * half_tok, half_tok, 0))
        part_o = y_swap(part)
        x_far = jnp.where(my == 0, jnp.concatenate([part, part_o], 0), jnp.concatenate([part_o, part], 0))
        x_far_mate = core_swap(x_far)

        def blocks(w, axis):
            mine = lax.dynamic_slice_in_dim(w, core * 128, 128, axis)
            theirs = lax.dynamic_slice_in_dim(w, (1 - core) * 128, 128, axis)
            return mine, core_swap(theirs)

        act0, act1 = blocks(w_act, 2)
        lin0, lin1 = blocks(w_lin, 2)
        down0, down1 = blocks(w_down, 1)
        router_mate = core_swap(w_router)

        positions = lengths[None, :] + jnp.arange(steps, dtype=jnp.int32)[:, None]
        inv_freq = ROPE_BASE ** (-(jnp.arange(hd // 2, dtype=F32) * 2.0 / hd))
        angles = positions.reshape(n_tok).astype(F32)[:, None] * inv_freq[None, :]
        cos, sin = jnp.cos(angles), jnp.sin(angles)
        cos2 = jnp.concatenate([cos, cos, cos, cos], axis=1)
        sin2 = jnp.concatenate([-sin, sin, -sin, sin], axis=1)

        qkv = qkv_call(me[None], (x_in, x_mate, x_far, x_far_mate), gain4, (w0, w1, w2, w3), cos2, sin2)
        acts = qkv.reshape(5, steps, batch, 256).transpose(2, 0, 1, 3).reshape(batch, 15, 256)
        acts = jnp.pad(acts, ((0, 0), (0, 1), (0, 0)))
        k_rows = k_cache.transpose(0, 2, 3, 1).reshape(batch * kv * hd, slots)
        v_rows = v_cache.transpose(0, 2, 3, 1).reshape(batch * kv * hd, slots)
        o, k_new, v_new = attn_call(lengths, acts, k_rows, v_rows)

        def back(rows):
            return rows.reshape(batch, kv, hd, slots).transpose(0, 3, 1, 2)

        wo = w_o.reshape(kv, group, hd, width).transpose(1, 0, 2, 3).reshape(group * kv * hd, width)
        x3 = x_in.reshape(steps, batch, width)
        o4 = o[:, : steps * group].reshape(batch, group, steps, 256)

        nbc = batch // NCHUNK
        outs = []
        for ci in range(NCHUNK):
            bs = slice(ci * nbc, (ci + 1) * nbc)
            nt = steps * nbc
            x_res = x3[:, bs].reshape(nt, width)
            oc = o4[bs].transpose(2, 0, 1, 3).reshape(nt, group * 256)
            proj = jnp.dot(oc, wo, preferred_element_type=F32).astype(BF16)
            proj_y = y_swap(proj)
            x1 = (x_res.astype(F32) + (proj.astype(F32) + proj_y.astype(F32))).astype(BF16)
            x1_mate = core_swap(x1)
            x1f, x1mf = x1.astype(F32), x1_mate.astype(F32)
            sq = jnp.sum(x1f * x1f, axis=-1) + jnp.sum(x1mf * x1mf, axis=-1)
            sq = sq + chip_swap(sq)
            scale = lax.rsqrt(sq / width_full + EPS)[:, None]
            h2 = jnp.concatenate([x1f * scale * gains[1], x1mf * scale * gains_c[1]], axis=1).astype(BF16)
            router = jnp.concatenate([w_router, router_mate], axis=0)
            logits = jnp.dot(h2, router, preferred_element_type=F32)
            chc = choices[:, bs].reshape(nt, 8)
            ch_rows = jnp.broadcast_to(chc.T.astype(BF16)[:, :, None], (8, nt, 128))
            keep, send = moe1_call(cx[None], h2, ch_rows, act0, lin0, act1, lin1)
            got = chip_swap(send)
            logits = logits + chip_swap(logits)
            picked = jnp.sum(jnp.where(chc[:, :, None] == jnp.arange(experts)[None, None, :], logits[:, None, :], 0.0), axis=-1)
            gate = jax.nn.softmax(picked, axis=-1)
            gate_mine = lax.dynamic_slice_in_dim(gate, cx * (nt // 2), nt // 2, 0).T
            hid = keep.astype(F32) + got.astype(F32)
            u = (gate_mine[:, :, None] * jax.nn.silu(hid[..., :128]) * hid[..., 128:]).astype(BF16)
            u_far = chip_swap(u)
            own, snd = moe2_call(cx[None], u, u_far, ch_rows, down0, down1)
            chip_sum = (own + core_swap(snd).astype(F32)).astype(BF16)
            moe = chip_sum.astype(F32) + y_swap(chip_sum).astype(F32)
            outs.append((x1.astype(F32) + moe).astype(BF16).reshape(steps, nbc, width))
        hidden = outs[0] if NCHUNK == 1 else jnp.concatenate(outs, axis=1)
        return hidden, back(k_new), back(v_new)

    return jax.shard_map(per_device, mesh=mesh, in_specs=in_specs, out_specs=out_specs, check_vma=False)
```

```python
import functools

import jax
import jax.numpy as jnp
from jax import lax
from jax.experimental import pallas as pl
from jax.experimental.pallas import tpu as pltpu
from jax.sharding import PartitionSpec as P


EPS = 1e-5
ROPE_BASE = 1.0e6
F32 = jnp.float32
BF16 = jnp.bfloat16
VMEM_LIMIT = 60 * 1024 * 1024
NB = 8


def cost(flops, moved):
    return pl.CostEstimate(flops=flops, bytes_accessed=moved, transcendentals=0)


def fixed(*shape):
    return pl.BlockSpec(shape, lambda *_: (0,) * len(shape))


def lead(*shape):
    return pl.BlockSpec(shape, lambda i, *_: (i,) + (0,) * (len(shape) - 1))


def norm_into(me, refs, tokens, hs):
    place = [me, me + 1 - 2 * (me % 2), (me + 2) % 4]
    place.append((place[1] + 2) % 4)
    rt = 128
    gains = [r[tokens : tokens + 1, :].astype(F32) for r in refs]

    def body(i, carry):
        rows = pl.ds(pl.multiple_of(i * rt, rt), rt)
        sq = []
        for r in refs:
            v = r[rows, :].astype(F32)
            sq.append(jnp.sum(v * v, axis=-1, keepdims=True))
        total = (sq[0] + sq[1]) + (sq[2] + sq[3])
        scale = lax.rsqrt(total / (4.0 * refs[0].shape[1]) + EPS)
        for n, r in enumerate(refs):
            hs[place[n], rows, :] = (r[rows, :].astype(F32) * scale * gains[n]).astype(BF16)
        return carry

    lax.fori_loop(0, tokens // rt, body, 0)


def project(me, hs, refs, ws, cos_ref, sin_ref, out_ref, turn):
    place = [me, me + 1 - 2 * (me % 2), (me + 2) % 4]
    place.append((place[1] + 2) % 4)
    for n, ref in enumerate(refs):
        ws[place[n]] = ref[0]
    low = lax.broadcasted_iota(jnp.int32, (1, 256), 1) % 64 < 32
    mt = 256
    for m in range(hs.shape[1] // mt):
        rows = slice(m * mt, (m + 1) * mt)
        acc = jnp.dot(hs[0, rows, :], ws[0], preferred_element_type=F32)
        for i in range(1, 4):
            acc += jnp.dot(hs[i, rows, :], ws[i], preferred_element_type=F32)
        v = acc.astype(BF16).astype(F32)
        other = jnp.where(low, pltpu.roll(v, 224, 1), pltpu.roll(v, 32, 1))
        cos, sin = cos_ref[rows, :], sin_ref[rows, :]
        if turn is not None:
            cos, sin = jnp.where(turn, cos, 1.0), jnp.where(turn, sin, 0.0)
        cos = jnp.concatenate([cos] * 2, axis=1)
        sin = jnp.concatenate([sin] * 2, axis=1)
        out_ref[0, rows, :] = (v * cos + other * sin).astype(BF16)


def qkv_a_kernel(me_ref, x0, x1, x2, x3, w0, w1, w2, w3, cos_ref, sin_ref, hs, out_ref, ws):
    @pl.when(pl.program_id(0) == 0)
    def _():
        norm_into(me_ref[0], (x0, x1, x2, x3), cos_ref.shape[0], hs)

    project(me_ref[0], hs, (w0, w1, w2, w3), ws, cos_ref, sin_ref, out_ref, None)


def qkv_b_kernel(me_ref, hs, w0, w1, w2, w3, cos_ref, sin_ref, before, out_ref, ws):
    project(me_ref[0], hs, (w0, w1, w2, w3), ws, cos_ref, sin_ref, out_ref, pl.program_id(0) < 2)


def qkv_calls(me, xs, was, wbs, cos, sin):
    tokens = cos.shape[0]
    rows, width = xs[0].shape
    na, nb = was[0].shape[0], wbs[0].shape[0]
    full = jax.ShapeDtypeStruct((na + nb, tokens, 256), BF16)
    w_spec = [lead(1, width, 256)] * 4
    t_spec = [fixed(tokens, 128)] * 2
    h_spec = fixed(4, tokens, width)
    params = pltpu.CompilerParams(vmem_limit_bytes=VMEM_LIMIT, dimension_semantics=("arbitrary",))
    h, first = pl.pallas_call(
        qkv_a_kernel,
        grid_spec=pltpu.PrefetchScalarGridSpec(
            num_scalar_prefetch=1,
            grid=(na,),
            in_specs=[fixed(rows, width)] * 4 + w_spec + t_spec,
            out_specs=[h_spec, lead(1, tokens, 256)],
            scratch_shapes=[pltpu.VMEM((4, width, 256), BF16)],
        ),
        out_shape=[jax.ShapeDtypeStruct((4, tokens, width), BF16), full],
        compiler_params=params,
        cost_estimate=cost(2 * tokens * width * 4 * 512, 6_000_000),
        name="qkv_a",
    )(me, *xs, *was, cos, sin)
    return pl.pallas_call(
        qkv_b_kernel,
        grid_spec=pltpu.PrefetchScalarGridSpec(
            num_scalar_prefetch=1,
            grid=(nb,),
            in_specs=[h_spec] + w_spec + t_spec + [pl.BlockSpec(memory_space=pl.ANY)],
            out_specs=pl.BlockSpec((1, tokens, 256), lambda i, m: (na + i, 0, 0)),
            scratch_shapes=[pltpu.VMEM((4, width, 256), BF16)],
        ),
        out_shape=full,
        input_output_aliases={8: 0},
        compiler_params=params,
        cost_estimate=cost(2 * tokens * width * 4 * 768, 6_000_000),
        name="qkv_b",
    )(me, h, *wbs, cos, sin, first)


def attn_kernel(off_ref, len_ref, a_ref, k_ref, v_ref, o_ref, lhs_ref, snew_ref, enew_ref):
    base = (off_ref[0] + pl.program_id(0)) * NB
    slot = lax.broadcasted_iota(jnp.int32, (1, 256), 1)
    block = slot // 64
    row = lax.broadcasted_iota(jnp.int32, (64, 128), 0) % 16 % 3
    col = lax.broadcasted_iota(jnp.int32, (64, 128), 1)
    every = a_ref[...].reshape(NB * 16, 256)
    scaled = every * jnp.bfloat16(0.125)
    for i in range(NB):
        q = scaled[i * 16 : i * 16 + 16]
        zero = jnp.zeros_like(q)
        lhs_ref[i * 64 : i * 64 + 64, :] = jnp.concatenate([jnp.where(block == k, q, zero) for k in range(4)], axis=0)
    snew_ref[...] = lax.dot_general(lhs_ref[...], every, (((1,), (1,)), ((), ())), preferred_element_type=F32)
    totals, mixes = [], []
    for i in range(NB):
        pos = len_ref[base + i]
        rows = slice(i * 64, i * 64 + 64)
        s_old = jnp.dot(lhs_ref[rows, :], k_ref[i * 256 : (i + 1) * 256, :], preferred_element_type=F32)
        fresh = (col >= i * 16 + 9) & (col <= row + (i * 16 + 9))
        s_old = jnp.where(slot < pos, s_old, -1.0e30)
        s_new = jnp.where(fresh, snew_ref[rows, :], -1.0e30)
        peak = jnp.max(jnp.maximum(jnp.maximum(s_old[:, :128], s_old[:, 128:]), s_new), axis=-1, keepdims=True)
        e_old = jnp.exp(s_old - peak)
        e_new = jnp.exp(s_new - peak)
        enew_ref[rows, :] = e_new.astype(BF16)
        total = jnp.sum(e_old[:, :128] + e_old[:, 128:] + e_new, axis=-1, keepdims=True)
        mixed = lax.dot_general(e_old.astype(BF16), v_ref[i * 256 : (i + 1) * 256, :], (((1,), (1,)), ((), ())), preferred_element_type=F32)
        res = mixed[0:16]
        tot = jnp.broadcast_to(total[0:16], (16, 256))
        for k in range(1, 4):
            part = slice(16 * k, 16 * k + 16)
            res = jnp.where(block == k, mixed[part], res)
            tot = jnp.where(block == k, total[part], tot)
        mixes.append(res)
        totals.append(tot)
    fresh_v = jnp.concatenate([every[3:], every[:3]], axis=0)
    extra = jnp.dot(enew_ref[...], fresh_v, preferred_element_type=F32)
    for i in range(NB):
        res = extra[i * 64 : i * 64 + 16]
        for k in range(1, 4):
            res = jnp.where(block == k, extra[i * 64 + 16 * k : i * 64 + 16 * k + 16], res)
        o_ref[i] = ((mixes[i] + res) / totals[i]).astype(BF16)


def attn_call(offset, lengths, acts, k_rows, v_rows, count):
    grid_spec = pltpu.PrefetchScalarGridSpec(
        num_scalar_prefetch=2,
        grid=(count // NB,),
        in_specs=[pl.BlockSpec((NB, 16, 256), lambda i, f, m: (f[0] + i, 0, 0))] + [pl.BlockSpec((NB * 256, 256), lambda i, f, m: (f[0] + i, 0))] * 2,
        out_specs=lead(NB, 16, 256),
        scratch_shapes=[pltpu.VMEM((NB * 64, 256), BF16), pltpu.VMEM((NB * 64, 128), F32), pltpu.VMEM((NB * 64, 128), BF16)],
    )
    return pl.pallas_call(
        attn_kernel,
        grid_spec=grid_spec,
        out_shape=jax.ShapeDtypeStruct((count, 16, 256), BF16),
        compiler_params=pltpu.CompilerParams(vmem_limit_bytes=VMEM_LIMIT, dimension_semantics=("arbitrary",)),
        cost_estimate=cost(count * 120_000_000, count * 262144),
        name="attn",
    )(offset, lengths, acts, k_rows, v_rows)


WB = 16
PIECES = (64, 96, 32, 64)


def write_kernel(start, aliased, len_ref, a_ref, k_ref, v_ref, *rest):
    ko_ref, vo_ref = rest[2:] if aliased else rest
    base = start + pl.program_id(0) * WB
    cols = jnp.transpose(a_ref[...].reshape(WB * 16, 256).astype(F32))
    slot = lax.broadcasted_iota(jnp.int32, (1, 256), 1)
    for i in range(WB):
        pos = len_ref[base + i]
        rows = slice(i * 256, (i + 1) * 256)
        hit = (slot >= pos) & (slot <= pos + 2)
        part = cols[:, (i // 8) * 128 : (i // 8) * 128 + 128]
        for first, src, dst in ((9, k_ref, ko_ref), (12, v_ref, vo_ref)):
            moved = pltpu.roll(part, (pos - (i % 8) * 16 - first + 256) % 128, 1).astype(BF16)
            for side in range(2):
                lanes = slice(side * 128, side * 128 + 128)
                dst[rows, lanes] = jnp.where(hit[:, lanes], moved, src[rows, lanes])


def write_call(start, count, lengths, acts, k_rows, v_rows, before):
    s0 = start // WB
    block = pl.BlockSpec((WB * 256, 256), lambda i, m: (s0 + i, 0))
    aliased = before is not None
    grid_spec = pltpu.PrefetchScalarGridSpec(
        num_scalar_prefetch=1,
        grid=(count // WB,),
        in_specs=[pl.BlockSpec((WB, 16, 256), lambda i, m: (s0 + i, 0, 0)), block, block]
        + ([pl.BlockSpec(memory_space=pl.ANY)] * 2 if aliased else []),
        out_specs=[block, block],
    )
    return pl.pallas_call(
        functools.partial(write_kernel, start, aliased),
        grid_spec=grid_spec,
        out_shape=[jax.ShapeDtypeStruct(k_rows.shape, BF16)] * 2,
        input_output_aliases={4: 0, 5: 1} if aliased else {},
        compiler_params=pltpu.CompilerParams(vmem_limit_bytes=VMEM_LIMIT, dimension_semantics=("arbitrary",)),
        cost_estimate=cost(count * 180_000_000, count * 524288),
        name="write",
    )(lengths, acts, k_rows, v_rows, *(before if aliased else ()))


E1 = 8


def moe1_kernel(half_ref, h_ref, ch_ref, a0, l0, a1, l1, out_ref, dense):
    step = pl.program_id(0)
    half = out_ref.shape[1]
    rt = 16

    @pl.when(step == 0)
    def _():
        out_ref[...] = jnp.zeros_like(out_ref)

    for g in range(E1 // 4):
        for k in range(4):
            e = g * 4 + k
            top = jnp.concatenate([a0[e], l0[e]], axis=1)
            low = jnp.concatenate([a1[e], l1[e]], axis=1)
            w = jnp.concatenate([top, low], axis=0)
            dense[g, k] = jnp.dot(h_ref[...], w, preferred_element_type=F32).astype(BF16)
        ids = [(step * E1 + g * 4 + k).astype(F32).astype(BF16) for k in range(4)]
        for i in range(half // rt):
            rows = slice(i * rt, (i + 1) * rt)
            d = [dense[g, k, rows, :] for k in range(4)]
            for j in range(8):
                chj = ch_ref[j, rows, :]
                hits = [chj == ids[k] for k in range(4)]
                for side in range(2):
                    lanes = slice(side * 128, side * 128 + 128)
                    acc = out_ref[j, rows, lanes]
                    for k in range(4):
                        acc = jnp.where(hits[k], d[k][:, lanes], acc)
                    out_ref[j, rows, lanes] = acc


def moe1_call(pick, h2, ch, w_act, w_lin, a1, l1):
    half = h2.shape[0] // 2
    experts, rows, _ = a1.shape
    mine = pl.BlockSpec((E1, rows, 128), lambda i, m: (i, 0, m[1]))
    theirs = lead(E1, rows, 128)
    grid_spec = pltpu.PrefetchScalarGridSpec(
        num_scalar_prefetch=1,
        grid=(experts // E1,),
        in_specs=[pl.BlockSpec((half, 2 * rows), lambda i, m: (m[0], 0)), pl.BlockSpec((8, half, 128), lambda i, m: (0, m[0], 0)), mine, mine, theirs, theirs],
        out_specs=fixed(8, half, 256),
        scratch_shapes=[pltpu.VMEM((E1 // 4, 4, half, 256), BF16)],
    )
    return pl.pallas_call(
        moe1_kernel,
        grid_spec=grid_spec,
        out_shape=jax.ShapeDtypeStruct((8, half, 256), BF16),
        compiler_params=pltpu.CompilerParams(vmem_limit_bytes=VMEM_LIMIT, dimension_semantics=("arbitrary",)),
        cost_estimate=cost(2 * half * 2 * rows * 256 * experts, 20_000_000),
        name="moe1",
    )(pick, h2, ch, w_act, w_lin, a1, l1)


E2 = 8


def moe2_kernel(half_ref, u_ref, ch_ref, wa, wb, own_ref, send_ref, spread, acc_ref):
    step = pl.program_id(0)
    half = u_ref.shape[1]
    width = wa.shape[2]
    rt = 16

    @pl.when(step == 0)
    def _():
        acc_ref[...] = jnp.zeros_like(acc_ref)

    prod = None
    for g in range(E2 // 4):
        ids = [(step * E2 + g * 4 + k).astype(F32).astype(BF16) for k in range(4)]
        for i in range(half // rt):
            rows = slice(i * rt, (i + 1) * rt)
            out = [jnp.zeros((rt, 128), BF16) for _ in range(4)]
            for j in range(8):
                chj = ch_ref[j, rows, :]
                uj = u_ref[j, rows, :]
                for k in range(4):
                    out[k] = jnp.where(chj == ids[k], uj, out[k])
            for k in range(4):
                spread[g, rows, k * 128 : (k + 1) * 128] = out[k]
        es = slice(g * 4, g * 4 + 4)
        w = jnp.concatenate([wa[es].reshape(512, width), wb[es].reshape(512, width)], axis=1)
        part = jnp.dot(spread[g], w, preferred_element_type=F32)
        prod = part if prod is None else prod + part
    acc_ref[...] += prod

    @pl.when(step == pl.num_programs(0) - 1)
    def _():
        own_ref[...] = acc_ref[:, :width]
        send_ref[...] = acc_ref[:, width:].astype(BF16)


def moe2_call(pick, u, ch, w_down, wb):
    half = u.shape[1]
    experts, rows, width = wb.shape
    grid_spec = pltpu.PrefetchScalarGridSpec(
        num_scalar_prefetch=1,
        grid=(experts // E2,),
        in_specs=[
            fixed(8, half, 128),
            pl.BlockSpec((8, half, 128), lambda i, m: (0, m[0], 0)),
            pl.BlockSpec((E2, rows, width), lambda i, m: (i, m[1], 0)),
            lead(E2, rows, width),
        ],
        out_specs=[fixed(half, width)] * 2,
        scratch_shapes=[pltpu.VMEM((E2 // 4, half, 512), BF16), pltpu.VMEM((half, 2 * width), F32)],
    )
    return pl.pallas_call(
        moe2_kernel,
        grid_spec=grid_spec,
        out_shape=[jax.ShapeDtypeStruct((half, width), F32), jax.ShapeDtypeStruct((half, width), BF16)],
        compiler_params=pltpu.CompilerParams(vmem_limit_bytes=VMEM_LIMIT, dimension_semantics=("arbitrary",)),
        cost_estimate=cost(2 * half * rows * 2 * width * experts, 10_000_000),
        name="moe2",
    )(pick, u, ch, w_down, wb)


def solution(mesh):
    cache_spec = P('dp', None, 'y', None)
    in_specs = (P(None, 'dp'), P('dp'), P(None, 'dp', None), P(None, 'x'), cache_spec, cache_spec, P('x'), P('x', 'y'), P('x', 'y'), P('x', 'y'), P('y', 'x'), P('x'), P('x', None), P(None, 'x', 'y'), P(None, 'x', 'y'), P(None, 'y', 'x'))
    out_specs = (P(None, 'dp', 'x'), cache_spec, cache_spec)

    def core_swap(v):
        return lax.ppermute(v, 'x', [(0, 1), (1, 0), (2, 3), (3, 2)])

    def chip_swap(v):
        return lax.ppermute(v, 'x', [(0, 2), (2, 0), (1, 3), (3, 1)])

    def y_swap(v):
        return lax.ppermute(v, 'y', [(0, 1), (1, 0)])

    def layer(tokens, lengths, choices, emb_table, k_cache, v_cache, g_attn, w_q, w_k, w_v, w_o, g_ffn, w_router, w_act, w_lin, w_down):
        steps, batch = tokens.shape
        width = emb_table.shape[1]
        kv, hd = k_cache.shape[2], k_cache.shape[3]
        slots = k_cache.shape[1]
        group = w_q.shape[1] // (kv * hd)
        experts = w_act.shape[0]
        width_full = width * 4
        me = lax.axis_index('x').astype(jnp.int32)
        my = lax.axis_index('y').astype(jnp.int32)
        core = me % 2
        cx = me // 2
        n_tok = steps * batch

        barrier = lax.optimization_barrier
        wq = w_q.reshape(width, kv, group, hd).transpose(2, 0, 1, 3).reshape(group, width, kv * hd)
        w_a = wq[:2]
        w_b = jnp.concatenate([wq[2:], w_k[None], w_v[None]], axis=0)
        half_tok = n_tok // 2
        x_in = jnp.take(emb_table, tokens.reshape(n_tok), axis=0, mode='clip')
        g_rows = jnp.concatenate([g_attn[None], g_ffn[None], jnp.zeros((14, width), BF16)], axis=0)
        x_ext = jnp.concatenate([x_in, g_rows])
        part = jnp.concatenate([lax.dynamic_slice_in_dim(x_in, my * half_tok, half_tok, 0), g_rows], axis=0)
        part, x_ext = barrier((part, x_ext))
        part = chip_swap(part)
        x_mate = core_swap(x_ext)
        wa2 = chip_swap(w_a)
        wb2 = chip_swap(w_b)

        def theirs(w, axis):
            return lax.dynamic_slice_in_dim(w, (1 - core) * 128, 128, axis)

        act_s = theirs(w_act, 2)
        lin_s, down_s = theirs(w_lin, 2), theirs(w_down, 1)
        part, act_s = barrier((part, act_s))
        part_o = y_swap(part[:half_tok])
        part_o, lin_s, down_s = barrier((part_o, lin_s, down_s))
        lo = jnp.where(my == 0, part[:half_tok], part_o)
        hi = jnp.where(my == 0, part_o, part[:half_tok])
        x_far = jnp.concatenate([lo, hi, part[half_tok:]])
        x_far_mate = core_swap(x_far)
        wa1, wb1, wa3 = core_swap(w_a), core_swap(w_b), core_swap(wa2)

        router = jnp.concatenate([w_router, core_swap(w_router)], axis=0)

        positions = lengths[None, :] + jnp.arange(steps, dtype=jnp.int32)[:, None]
        inv_freq = ROPE_BASE ** (-(jnp.arange(hd // 2, dtype=F32) * 2.0 / hd))
        angles = positions.reshape(n_tok).astype(F32)[:, None] * inv_freq[None, :]
        cos, sin = jnp.cos(angles), jnp.sin(angles)
        cos2, sin2 = jnp.tile(cos, (1, 4)), jnp.tile(jnp.concatenate([-sin, sin], axis=1), (1, 2))
        choice_rows = choices.reshape(n_tok, 8)
        ch_rows = jnp.broadcast_to(choice_rows.T.astype(BF16)[:, :, None], (8, n_tok, 128))
        wo = w_o.reshape(kv, group, hd, width).transpose(1, 0, 2, 3).reshape(group * kv * hd, width)

        pick_m, pick_f = jnp.stack([cx, core]), jnp.stack([1 - cx, core])
        offset = (core * (batch // 2) // NB)[None]
        wb2, ch_rows, wo, pick_m, pick_f, offset = barrier((wb2, ch_rows, wo, pick_m, pick_f, offset))
        wb3 = core_swap(wb2)
        act1, lin1, down1 = core_swap(act_s), core_swap(lin_s), core_swap(down_s)
        qkv = qkv_calls(me[None], (x_ext, x_mate, x_far, x_far_mate), (w_a, wa1, wa2, wa3), (w_b, wb1, wb2, wb3), cos2, sin2)
        acts = qkv.reshape(5, steps, batch, 256).transpose(2, 0, 1, 3).reshape(batch, 15, 256)
        acts = jnp.pad(acts, ((0, 0), (0, 1), (0, 0)))
        k_rows = k_cache.transpose(0, 2, 3, 1).reshape(batch * kv * hd, slots)
        v_rows = v_cache.transpose(0, 2, 3, 1).reshape(batch * kv * hd, slots)
        starts = [sum(PIECES[:i]) for i in range(len(PIECES))]

        def write(i, acts, before):
            return tuple(write_call(starts[i], PIECES[i], lengths, acts, k_rows, v_rows, before))

        def back(rows):
            return rows.reshape(batch, kv, hd, slots).transpose(0, 3, 1, 2)

        o = attn_call(offset, lengths, acts, k_rows, v_rows, batch // 2)[:, : steps * group]
        o_mate = core_swap(o)
        o = jnp.where(core == 0, jnp.concatenate([o, o_mate]), jnp.concatenate([o_mate, o]))
        oc = o.reshape(batch, group, steps, 256).transpose(2, 0, 1, 3).reshape(n_tok, group * 256)
        proj = jnp.dot(oc, wo, preferred_element_type=F32).astype(BF16)

        proj, acts = barrier((proj, acts))
        proj_y = y_swap(proj)
        caches = write(0, acts, None)
        proj_y, caches = barrier((proj_y, caches))

        x1 = (x_in.astype(F32) + (proj.astype(F32) + proj_y.astype(F32))).astype(BF16)
        x1_mate = core_swap(x1)
        x1f, x1mf = x1.astype(F32), x1_mate.astype(F32)
        sq = jnp.sum(x1f * x1f, axis=-1) + jnp.sum(x1mf * x1mf, axis=-1)
        sq = sq + chip_swap(sq)
        scale = lax.rsqrt(sq / width_full + EPS)[:, None]
        g_own, g_mate = g_ffn.astype(F32), x_mate[n_tok + 1].astype(F32)
        h2 = jnp.concatenate([x1f * scale * g_own, x1mf * scale * g_mate], axis=1).astype(BF16)
        logits = jnp.dot(h2, router, preferred_element_type=F32)

        send = moe1_call(pick_f, h2, ch_rows, w_act, w_lin, act1, lin1)
        send, h2, acts = barrier((send, h2, acts))
        got = chip_swap(send)
        keep = moe1_call(pick_m, h2, ch_rows, w_act, w_lin, act1, lin1)
        caches = write(1, acts, caches)
        logits = logits + chip_swap(logits)
        picked = jnp.sum(jnp.where(choice_rows[:, :, None] == jnp.arange(experts)[None, None, :], logits[:, None, :], 0.0), axis=-1)
        gate = jax.nn.softmax(picked, axis=-1)
        gate_mine = lax.dynamic_slice_in_dim(gate, cx * half_tok, half_tok, 0).T
        got, caches, gate_mine = barrier((got, caches, gate_mine))
        hid = keep.astype(F32) + got.astype(F32)
        u = (gate_mine[:, :, None] * jax.nn.silu(hid[..., :128]) * hid[..., 128:]).astype(BF16)

        u, acts = barrier((u, acts))
        u_far = chip_swap(u)
        own_m, snd_m = moe2_call(pick_m, u, ch_rows, w_down, down1)
        caches = write(2, acts, caches)
        u_far, caches, acts, snd_m = barrier((u_far, caches, acts, snd_m))
        sum_m = (own_m + core_swap(snd_m).astype(F32)).astype(BF16)
        sum_m_y = y_swap(sum_m)
        own_f, snd_f = moe2_call(pick_f, u_far, ch_rows, w_down, down1)
        snd_f, acts = barrier((snd_f, acts))
        sum_f = (own_f + core_swap(snd_f).astype(F32)).astype(BF16)
        sum_f_y = y_swap(sum_f)
        caches = write(3, acts, caches)
        sum_f_y, caches = barrier((sum_f_y, caches))
        moe_m = sum_m.astype(F32) + sum_m_y.astype(F32)
        moe_f = sum_f.astype(F32) + sum_f_y.astype(F32)
        moe = jnp.where(cx == 0, jnp.concatenate([moe_m, moe_f]), jnp.concatenate([moe_f, moe_m]))
        hidden = (x1.astype(F32) + moe).astype(BF16).reshape(steps, batch, width)
        k_new, v_new = caches
        return hidden, back(k_new), back(v_new)

    return jax.shard_map(layer, mesh=mesh, in_specs=in_specs, out_specs=out_specs, check_vma=False)
```

```python
import functools

import jax
import jax.numpy as jnp
from jax import lax
from jax.experimental import pallas as pl
from jax.experimental.pallas import tpu as pltpu
from jax.sharding import PartitionSpec as P


EPS = 1e-5
ROPE_BASE = 1.0e6
F32 = jnp.float32
BF16 = jnp.bfloat16
VMEM_LIMIT = 60 * 1024 * 1024
LANE = 128
WIDE = 256
NB = 8


def cost(flops, moved):
    return pl.CostEstimate(flops=flops, bytes_accessed=moved, transcendentals=0)


def fixed(*shape):
    return pl.BlockSpec(shape, lambda *_: (0,) * len(shape))


def lead(*shape):
    return pl.BlockSpec(shape, lambda i, *_: (i,) + (0,) * (len(shape) - 1))


def norm_into(me, refs, tokens, hs):
    place = [me, me + 1 - 2 * (me % 2), (me + 2) % 4]
    place.append((place[1] + 2) % 4)
    rt = LANE
    width = refs[0].shape[1]
    gains = [r[tokens : tokens + 1, :].astype(F32) for r in refs]

    def body(i, carry):
        rows = pl.ds(pl.multiple_of(i * rt, rt), rt)
        sq = []
        for r in refs:
            v = r[rows, :].astype(F32)
            sq.append(jnp.sum(v * v, axis=-1, keepdims=True))
        total = (sq[0] + sq[1]) + (sq[2] + sq[3])
        scale = lax.rsqrt(total / (4.0 * refs[0].shape[1]) + EPS)
        for n, r in enumerate(refs):
            hs[rows, pl.ds(pl.multiple_of(place[n] * width, LANE), width)] = (r[rows, :].astype(F32) * scale * gains[n]).astype(BF16)
        return carry

    lax.fori_loop(0, tokens // rt, body, 0)


def project(me, hs, refs, ws, cos_ref, sin_ref, out_ref, turn):
    place = [me, me + 1 - 2 * (me % 2), (me + 2) % 4]
    place.append((place[1] + 2) % 4)
    for n, ref in enumerate(refs):
        ws[pl.ds(pl.multiple_of(place[n] * ref.shape[1], LANE), ref.shape[1]), :] = ref[0]
    low = lax.broadcasted_iota(jnp.int32, (1, WIDE), 1) % 64 < 32
    mt = hs.shape[0]
    for m in range(hs.shape[0] // mt):
        rows = slice(m * mt, (m + 1) * mt)
        acc = jnp.dot(hs[rows, :], ws[...], preferred_element_type=F32)
        v = acc.astype(BF16).astype(F32)
        other = jnp.where(low, pltpu.roll(v, 224, 1), pltpu.roll(v, 32, 1))
        cos, sin = cos_ref[rows, :], sin_ref[rows, :]
        if turn is not None:
            cos, sin = jnp.where(turn, cos, 1.0), jnp.where(turn, sin, 0.0)
        cos = jnp.concatenate([cos] * 2, axis=1)
        sin = jnp.concatenate([sin] * 2, axis=1)
        out_ref[0, rows, :] = (v * cos + other * sin).astype(BF16)


def qkv_a_kernel(me_ref, x0, x1, x2, x3, w0, w1, w2, w3, cos_ref, sin_ref, hs, out_ref, ws):
    @pl.when(pl.program_id(0) == 0)
    def _():
        norm_into(me_ref[0], (x0, x1, x2, x3), cos_ref.shape[0], hs)

    project(me_ref[0], hs, (w0, w1, w2, w3), ws, cos_ref, sin_ref, out_ref, None)


def qkv_b_kernel(me_ref, hs, w0, w1, w2, w3, cos_ref, sin_ref, before, out_ref, ws):
    project(me_ref[0], hs, (w0, w1, w2, w3), ws, cos_ref, sin_ref, out_ref, pl.program_id(0) < 2)


def qkv_calls(me, xs, was, wbs, cos, sin):
    tokens = cos.shape[0]
    rows, width = xs[0].shape
    na, nb = was[0].shape[0], wbs[0].shape[0]
    full = jax.ShapeDtypeStruct((na + nb, tokens, WIDE), BF16)
    w_spec = [lead(1, width, WIDE)] * 4
    t_spec = [fixed(tokens, LANE)] * 2
    h_spec = fixed(tokens, 4 * width)
    params = pltpu.CompilerParams(vmem_limit_bytes=VMEM_LIMIT, dimension_semantics=("arbitrary",))
    h, first = pl.pallas_call(
        qkv_a_kernel,
        grid_spec=pltpu.PrefetchScalarGridSpec(
            num_scalar_prefetch=1,
            grid=(na,),
            in_specs=[fixed(rows, width)] * 4 + w_spec + t_spec,
            out_specs=[h_spec, lead(1, tokens, WIDE)],
            scratch_shapes=[pltpu.VMEM((4 * width, WIDE), BF16)],
        ),
        out_shape=[jax.ShapeDtypeStruct((tokens, 4 * width), BF16), full],
        compiler_params=params,
        cost_estimate=cost(2 * tokens * width * 4 * 512, 6_000_000),
        name="qkv_a",
    )(me, *xs, *was, cos, sin)
    return pl.pallas_call(
        qkv_b_kernel,
        grid_spec=pltpu.PrefetchScalarGridSpec(
            num_scalar_prefetch=1,
            grid=(nb,),
            in_specs=[h_spec] + w_spec + t_spec + [pl.BlockSpec(memory_space=pl.ANY)],
            out_specs=pl.BlockSpec((1, tokens, WIDE), lambda i, m: (na + i, 0, 0)),
            scratch_shapes=[pltpu.VMEM((4 * width, WIDE), BF16)],
        ),
        out_shape=full,
        input_output_aliases={8: 0},
        compiler_params=params,
        cost_estimate=cost(2 * tokens * width * 4 * 768, 6_000_000),
        name="qkv_b",
    )(me, h, *wbs, cos, sin, first)


def by_sequence(a_ref, rows_ref, turned_ref):
    kinds, count, _ = a_ref.shape
    for side in range(2):
        lanes = slice(side * LANE, side * LANE + LANE)
        for r in range(kinds):
            rows_ref[side, r * count : (r + 1) * count, :] = a_ref[r, :, lanes].astype(F32)
        rows_ref[side, kinds * count :, :] = jnp.zeros((count, LANE), F32)
        for i in range(count):
            turned_ref[i * 16 : i * 16 + 16, lanes] = rows_ref[side, pl.ds(i, 16, stride=count), :].astype(turned_ref.dtype)


def attn_kernel(off_ref, len_ref, a_ref, k_ref, k2_ref, v_ref, v2_ref, o_ref, lhs_ref, snew_ref, enew_ref, rows_ref, turned_ref):
    base = (off_ref[0] + pl.program_id(0)) * NB
    slot = lax.broadcasted_iota(jnp.int32, (1, WIDE), 1)
    block = slot // 64
    row = lax.broadcasted_iota(jnp.int32, (64, LANE), 0) % 16 % 3
    col = lax.broadcasted_iota(jnp.int32, (64, LANE), 1)
    by_sequence(a_ref, rows_ref, turned_ref)
    every = turned_ref[...]
    scaled = every * jnp.bfloat16(0.125)
    for i in range(NB):
        q = scaled[i * 16 : i * 16 + 16]
        zero = jnp.zeros_like(q)
        lhs_ref[i * 64 : i * 64 + 64, :] = jnp.concatenate([jnp.where(block == k, q, zero) for k in range(4)], axis=0)
    snew_ref[...] = lax.dot_general(lhs_ref[...], every, (((1,), (1,)), ((), ())), preferred_element_type=F32)
    totals, mixes = [], []
    for i in range(NB):
        pos = len_ref[base + i]
        rows = slice(i * 64, i * 64 + 64)
        s_old = jnp.dot(lhs_ref[rows, :], (k_ref, k2_ref)[i // 4][i % 4 * WIDE : (i % 4 + 1) * WIDE, :], preferred_element_type=F32)
        fresh = (col >= i * 16 + 9) & (col <= row + (i * 16 + 9))
        s_old = jnp.where(slot < pos, s_old, -1.0e30)
        s_new = jnp.where(fresh, snew_ref[rows, :], -1.0e30)
        peak = jnp.max(jnp.maximum(jnp.maximum(s_old[:, :LANE], s_old[:, LANE:]), s_new), axis=-1, keepdims=True)
        e_old = jnp.exp(s_old - peak)
        e_new = jnp.exp(s_new - peak)
        enew_ref[rows, :] = e_new.astype(BF16)
        total = jnp.sum(e_old[:, :LANE] + e_old[:, LANE:] + e_new, axis=-1, keepdims=True)
        mixed = lax.dot_general(e_old.astype(BF16), (v_ref, v2_ref)[i // 4][i % 4 * WIDE : (i % 4 + 1) * WIDE, :], (((1,), (1,)), ((), ())), preferred_element_type=F32)
        res = mixed[0:16]
        tot = jnp.broadcast_to(total[0:16], (16, WIDE))
        for k in range(1, 4):
            part = slice(16 * k, 16 * k + 16)
            res = jnp.where(block == k, mixed[part], res)
            tot = jnp.where(block == k, total[part], tot)
        mixes.append(res)
        totals.append(tot)
    fresh_v = jnp.concatenate([every[3:], every[:3]], axis=0)
    extra = jnp.dot(enew_ref[...], fresh_v, preferred_element_type=F32)
    for i in range(NB):
        res = extra[i * 64 : i * 64 + 16]
        for k in range(1, 4):
            res = jnp.where(block == k, extra[i * 64 + 16 * k : i * 64 + 16 * k + 16], res)
        o_ref[i] = ((mixes[i] + res) / totals[i]).astype(BF16)


def attn_call(offset, lengths, acts, k_rows, v_rows, count):
    even = pl.BlockSpec((NB * LANE, WIDE), lambda i, f, m: (2 * (f[0] + i), 0))
    odd = pl.BlockSpec((NB * LANE, WIDE), lambda i, f, m: (2 * (f[0] + i) + 1, 0))
    grid_spec = pltpu.PrefetchScalarGridSpec(
        num_scalar_prefetch=2,
        grid=(count // NB,),
        in_specs=[pl.BlockSpec((15, NB, WIDE), lambda i, f, m: (0, f[0] + i, 0)), even, odd, even, odd],
        out_specs=lead(NB, 16, WIDE),
        scratch_shapes=[pltpu.VMEM((NB * 64, WIDE), BF16), pltpu.VMEM((NB * 64, LANE), F32), pltpu.VMEM((NB * 64, LANE), BF16), pltpu.VMEM((2, NB * 16, LANE), F32), pltpu.VMEM((NB * 16, WIDE), BF16)],
    )
    return pl.pallas_call(
        attn_kernel,
        grid_spec=grid_spec,
        out_shape=jax.ShapeDtypeStruct((count, 16, WIDE), BF16),
        compiler_params=pltpu.CompilerParams(vmem_limit_bytes=VMEM_LIMIT, dimension_semantics=("arbitrary",)),
        cost_estimate=cost(count * 120_000_000, count * 262144),
        name="attn",
    )(offset, lengths, acts, k_rows, k_rows, v_rows, v_rows)


WB = 16
PIECES = (48, 64, 80, 32, 32)


def write_kernel(start, aliased, len_ref, a_ref, k_ref, v_ref, *rest):
    ko_ref, vo_ref, rows_ref, turned_ref = rest[2:] if aliased else rest
    by_sequence(a_ref, rows_ref, turned_ref)
    base = start + pl.program_id(0) * WB
    cols = jnp.transpose(turned_ref[...])
    slot = lax.broadcasted_iota(jnp.int32, (1, WIDE), 1)
    for i in range(WB):
        pos = len_ref[base + i]
        rows = slice(i * WIDE, (i + 1) * WIDE)
        hit = (slot >= pos) & (slot <= pos + 2)
        part = cols[:, (i // 8) * LANE : (i // 8) * LANE + LANE]
        for first, src, dst in ((9, k_ref, ko_ref), (12, v_ref, vo_ref)):
            moved = pltpu.roll(part, (pos - (i % 8) * 16 - first + WIDE) % LANE, 1).astype(BF16)
            for side in range(2):
                lanes = slice(side * LANE, side * LANE + LANE)
                dst[rows, lanes] = jnp.where(hit[:, lanes], moved, src[rows, lanes])


def write_call(start, count, lengths, acts, k_rows, v_rows, before):
    s0 = start // WB
    block = pl.BlockSpec((WB * WIDE, WIDE), lambda i, m: (s0 + i, 0))
    aliased = before is not None
    grid_spec = pltpu.PrefetchScalarGridSpec(
        num_scalar_prefetch=1,
        grid=(count // WB,),
        in_specs=[pl.BlockSpec((15, WB, WIDE), lambda i, m: (0, s0 + i, 0)), block, block]
        + ([pl.BlockSpec(memory_space=pl.ANY)] * 2 if aliased else []),
        out_specs=[block, block],
        scratch_shapes=[pltpu.VMEM((2, WB * 16, LANE), F32), pltpu.VMEM((WB * 16, WIDE), F32)],
    )
    return pl.pallas_call(
        functools.partial(write_kernel, start, aliased),
        grid_spec=grid_spec,
        out_shape=[jax.ShapeDtypeStruct(k_rows.shape, BF16)] * 2,
        input_output_aliases={4: 0, 5: 1} if aliased else {},
        compiler_params=pltpu.CompilerParams(vmem_limit_bytes=VMEM_LIMIT, dimension_semantics=("arbitrary",)),
        cost_estimate=cost(count * 180_000_000, count * 524288),
        name="write",
    )(lengths, acts, k_rows, v_rows, *(before if aliased else ()))


E1 = 8


def moe1_kernel(half_ref, h_ref, ch_ref, a0, l0, a1, l1, out_ref, dense):
    step = pl.program_id(0)
    half = out_ref.shape[1]
    rt = 16

    @pl.when(step == 0)
    def _():
        out_ref[...] = jnp.zeros_like(out_ref)

    for g in range(E1 // 4):
        for k in range(4):
            e = g * 4 + k
            top = jnp.concatenate([a0[e], l0[e]], axis=1)
            low = jnp.concatenate([a1[e], l1[e]], axis=1)
            w = jnp.concatenate([top, low], axis=0)
            dense[g, k] = jnp.dot(h_ref[...], w, preferred_element_type=F32).astype(BF16)
        ids = [(step * E1 + g * 4 + k).astype(F32).astype(BF16) for k in range(4)]
        for i in range(half // rt):
            rows = slice(i * rt, (i + 1) * rt)
            d = [dense[g, k, rows, :] for k in range(4)]
            for j in range(8):
                chj = ch_ref[j, rows, :]
                hits = [chj == ids[k] for k in range(4)]
                for side in range(2):
                    lanes = slice(side * LANE, side * LANE + LANE)
                    acc = out_ref[j, rows, lanes]
                    for k in range(4):
                        acc = jnp.where(hits[k], d[k][:, lanes], acc)
                    out_ref[j, rows, lanes] = acc


def moe1_call(pick, h2, ch, w_act, w_lin, a1, l1):
    half = h2.shape[0] // 2
    experts, rows, _ = a1.shape
    mine = pl.BlockSpec((E1, rows, LANE), lambda i, m: (i, 0, m[1]))
    theirs = lead(E1, rows, LANE)
    grid_spec = pltpu.PrefetchScalarGridSpec(
        num_scalar_prefetch=1,
        grid=(experts // E1,),
        in_specs=[pl.BlockSpec((half, 2 * rows), lambda i, m: (m[0], 0)), pl.BlockSpec((8, half, LANE), lambda i, m: (0, m[0], 0)), mine, mine, theirs, theirs],
        out_specs=fixed(8, half, WIDE),
        scratch_shapes=[pltpu.VMEM((E1 // 4, 4, half, WIDE), BF16)],
    )
    return pl.pallas_call(
        moe1_kernel,
        grid_spec=grid_spec,
        out_shape=jax.ShapeDtypeStruct((8, half, WIDE), BF16),
        compiler_params=pltpu.CompilerParams(vmem_limit_bytes=VMEM_LIMIT, dimension_semantics=("arbitrary",)),
        cost_estimate=cost(2 * half * 2 * rows * WIDE * experts, 20_000_000),
        name="moe1",
    )(pick, h2, ch, w_act, w_lin, a1, l1)


E2 = 8


def moe2_kernel(half_ref, u_ref, ch_ref, wa, wb, own_ref, send_ref, spread, acc_ref):
    step = pl.program_id(0)
    half = u_ref.shape[1]
    width = wa.shape[2]
    rt = 16

    @pl.when(step == 0)
    def _():
        acc_ref[...] = jnp.zeros_like(acc_ref)

    prod = None
    for g in range(E2 // 4):
        ids = [(step * E2 + g * 4 + k).astype(F32).astype(BF16) for k in range(4)]
        for i in range(half // rt):
            rows = slice(i * rt, (i + 1) * rt)
            out = [jnp.zeros((rt, LANE), BF16) for _ in range(4)]
            for j in range(8):
                chj = ch_ref[j, rows, :]
                uj = u_ref[j, rows, :]
                for k in range(4):
                    out[k] = jnp.where(chj == ids[k], uj, out[k])
            for k in range(4):
                spread[g, rows, k * LANE : (k + 1) * LANE] = out[k]
        es = slice(g * 4, g * 4 + 4)
        w = jnp.concatenate([wa[es].reshape(512, width), wb[es].reshape(512, width)], axis=1)
        part = jnp.dot(spread[g], w, preferred_element_type=F32)
        prod = part if prod is None else prod + part
    acc_ref[...] += prod

    @pl.when(step == pl.num_programs(0) - 1)
    def _():
        own_ref[...] = acc_ref[:, :width]
        send_ref[...] = acc_ref[:, width:].astype(BF16)


def moe2_call(pick, u, ch, w_down, wb):
    half = u.shape[1]
    experts, rows, width = wb.shape
    grid_spec = pltpu.PrefetchScalarGridSpec(
        num_scalar_prefetch=1,
        grid=(experts // E2,),
        in_specs=[
            fixed(8, half, LANE),
            pl.BlockSpec((8, half, LANE), lambda i, m: (0, m[0], 0)),
            pl.BlockSpec((E2, rows, width), lambda i, m: (i, m[1], 0)),
            lead(E2, rows, width),
        ],
        out_specs=[fixed(half, width)] * 2,
        scratch_shapes=[pltpu.VMEM((E2 // 4, half, 512), BF16), pltpu.VMEM((half, 2 * width), F32)],
    )
    return pl.pallas_call(
        moe2_kernel,
        grid_spec=grid_spec,
        out_shape=[jax.ShapeDtypeStruct((half, width), F32), jax.ShapeDtypeStruct((half, width), BF16)],
        compiler_params=pltpu.CompilerParams(vmem_limit_bytes=VMEM_LIMIT, dimension_semantics=("arbitrary",)),
        cost_estimate=cost(2 * half * rows * 2 * width * experts, 10_000_000),
        name="moe2",
    )(pick, u, ch, w_down, wb)


def solution(mesh):
    cache_spec = P('dp', None, 'y', None)
    in_specs = (P(None, 'dp'), P('dp'), P(None, 'dp', None), P(None, 'x'), cache_spec, cache_spec, P('x'), P('x', 'y'), P('x', 'y'), P('x', 'y'), P('y', 'x'), P('x'), P('x', None), P(None, 'x', 'y'), P(None, 'x', 'y'), P(None, 'y', 'x'))
    out_specs = (P(None, 'dp', 'x'), cache_spec, cache_spec)

    def core_swap(v):
        return lax.ppermute(v, 'x', [(0, 1), (1, 0), (2, 3), (3, 2)])

    def chip_swap(v):
        return lax.ppermute(v, 'x', [(0, 2), (2, 0), (1, 3), (3, 1)])

    def y_swap(v):
        return lax.ppermute(v, 'y', [(0, 1), (1, 0)])

    def layer(tokens, lengths, choices, emb_table, k_cache, v_cache, g_attn, w_q, w_k, w_v, w_o, g_ffn, w_router, w_act, w_lin, w_down):
        steps, batch = tokens.shape
        width = emb_table.shape[1]
        kv, hd = k_cache.shape[2], k_cache.shape[3]
        slots = k_cache.shape[1]
        group = w_q.shape[1] // (kv * hd)
        experts = w_act.shape[0]
        width_full = width * 4
        me = lax.axis_index('x').astype(jnp.int32)
        my = lax.axis_index('y').astype(jnp.int32)
        core = me % 2
        cx = me // 2
        n_tok = steps * batch

        barrier = lax.optimization_barrier
        wq = w_q.reshape(width, kv, group, hd).transpose(2, 0, 1, 3).reshape(group, width, kv * hd)
        w_a = wq[:2]
        w_b = jnp.concatenate([wq[2:], w_k[None], w_v[None]], axis=0)
        half_tok = n_tok // 2
        x_in = jnp.take(emb_table, tokens.reshape(n_tok), axis=0, mode='clip')
        g_rows = jnp.concatenate([g_attn[None], g_ffn[None], jnp.zeros((14, width), BF16)], axis=0)
        x_ext = jnp.concatenate([x_in, g_rows])
        part = jnp.concatenate([lax.dynamic_slice_in_dim(x_in, my * half_tok, half_tok, 0), g_rows], axis=0)
        part, x_ext = barrier((part, x_ext))
        part = chip_swap(part)
        x_mate = core_swap(x_ext)
        wa2 = chip_swap(w_a)
        wb2 = chip_swap(w_b)

        def theirs(w, axis):
            return lax.dynamic_slice_in_dim(w, (1 - core) * LANE, LANE, axis)

        act_s = theirs(w_act, 2)
        lin_s, down_s = theirs(w_lin, 2), theirs(w_down, 1)
        part, act_s = barrier((part, act_s))
        part_o = y_swap(part[:half_tok])
        part_o, lin_s, down_s = barrier((part_o, lin_s, down_s))
        lo = jnp.where(my == 0, part[:half_tok], part_o)
        hi = jnp.where(my == 0, part_o, part[:half_tok])
        x_far = jnp.concatenate([lo, hi, part[half_tok:]])
        x_far_mate = core_swap(x_far)
        wa1, wb1, wa3 = core_swap(w_a), core_swap(w_b), core_swap(wa2)

        router = jnp.concatenate([w_router, core_swap(w_router)], axis=0)

        positions = lengths[None, :] + jnp.arange(steps, dtype=jnp.int32)[:, None]
        inv_freq = ROPE_BASE ** (-(jnp.arange(hd // 2, dtype=F32) * 2.0 / hd))
        angles = positions.reshape(n_tok).astype(F32)[:, None] * inv_freq[None, :]
        cos, sin = jnp.cos(angles), jnp.sin(angles)
        cos2, sin2 = jnp.tile(cos, (1, 4)), jnp.tile(jnp.concatenate([-sin, sin], axis=1), (1, 2))
        choice_rows = choices.reshape(n_tok, 8)
        ch_rows = jnp.broadcast_to(choice_rows.T.astype(BF16)[:, :, None], (8, n_tok, LANE))
        wo = w_o.reshape(kv, group, hd, width).transpose(1, 0, 2, 3).reshape(group * kv * hd, width)

        pick_m, pick_f = jnp.stack([cx, core]), jnp.stack([1 - cx, core])
        offset = (me * (batch // 4) // NB)[None]
        wb2, ch_rows, wo, pick_m, pick_f, offset = barrier((wb2, ch_rows, wo, pick_m, pick_f, offset))
        wb3 = core_swap(wb2)
        act1, lin1, down1 = core_swap(act_s), core_swap(lin_s), core_swap(down_s)
        qkv = qkv_calls(me[None], (x_ext, x_mate, x_far, x_far_mate), (w_a, wa1, wa2, wa3), (w_b, wb1, wb2, wb3), cos2, sin2)
        acts = qkv.reshape(5 * steps, batch, WIDE)
        k_rows = k_cache.transpose(0, 2, 3, 1).reshape(batch * kv * hd, slots)
        v_rows = v_cache.transpose(0, 2, 3, 1).reshape(batch * kv * hd, slots)
        starts = [sum(PIECES[:i]) for i in range(len(PIECES))]

        def write(i, acts, before):
            return tuple(write_call(starts[i], PIECES[i], lengths, acts, k_rows, v_rows, before))

        def back(rows):
            return rows.reshape(batch, kv, hd, slots).transpose(0, 3, 1, 2)

        o = attn_call(offset, lengths, acts, k_rows, v_rows, batch // 4)[:, : steps * group]
        o, acts = barrier((o, acts))
        o_far = chip_swap(o)
        caches = write(0, acts, None)
        o_far, caches = barrier((o_far, caches))

        def in_order(v, mate):
            return jnp.where(core == 0, jnp.concatenate([v, mate]), jnp.concatenate([mate, v]))

        near, far = in_order(o, core_swap(o)), in_order(o_far, core_swap(o_far))
        o = jnp.where(cx == 0, jnp.concatenate([near, far]), jnp.concatenate([far, near]))
        oc = o.reshape(batch, group, steps, WIDE).transpose(2, 0, 1, 3).reshape(n_tok, group * WIDE)
        proj = jnp.dot(oc, wo, preferred_element_type=F32).astype(BF16)

        proj, acts = barrier((proj, acts))
        proj_y = y_swap(proj)
        caches = write(1, acts, caches)
        proj_y, caches = barrier((proj_y, caches))

        x1 = (x_in.astype(F32) + (proj.astype(F32) + proj_y.astype(F32))).astype(BF16)
        x1_mate = core_swap(x1)
        x1f, x1mf = x1.astype(F32), x1_mate.astype(F32)
        sq = jnp.sum(x1f * x1f, axis=-1) + jnp.sum(x1mf * x1mf, axis=-1)
        sq = sq + chip_swap(sq)
        scale = lax.rsqrt(sq / width_full + EPS)[:, None]
        g_own, g_mate = g_ffn.astype(F32), x_mate[n_tok + 1].astype(F32)
        h2 = jnp.concatenate([x1f * scale * g_own, x1mf * scale * g_mate], axis=1).astype(BF16)
        logits = jnp.dot(h2, router, preferred_element_type=F32)

        send = moe1_call(pick_f, h2, ch_rows, w_act, w_lin, act1, lin1)
        send, h2, acts = barrier((send, h2, acts))
        got = chip_swap(send)
        keep = moe1_call(pick_m, h2, ch_rows, w_act, w_lin, act1, lin1)
        caches = write(2, acts, caches)
        logits = logits + chip_swap(logits)
        picked = jnp.sum(jnp.where(choice_rows[:, :, None] == jnp.arange(experts)[None, None, :], logits[:, None, :], 0.0), axis=-1)
        gate = jax.nn.softmax(picked, axis=-1)
        gate_mine = lax.dynamic_slice_in_dim(gate, cx * half_tok, half_tok, 0).T
        got, caches, gate_mine = barrier((got, caches, gate_mine))
        hid = keep.astype(F32) + got.astype(F32)
        u = (gate_mine[:, :, None] * jax.nn.silu(hid[..., :LANE]) * hid[..., LANE:]).astype(BF16)

        u, acts = barrier((u, acts))
        u_far = chip_swap(u)
        own_m, snd_m = moe2_call(pick_m, u, ch_rows, w_down, down1)
        caches = write(3, acts, caches)
        sum_m = (own_m + core_swap(snd_m).astype(F32)).astype(BF16)
        u_far, caches, acts, sum_m = barrier((u_far, caches, acts, sum_m))
        sum_m_y = y_swap(sum_m)
        own_f, snd_f = moe2_call(pick_f, u_far, ch_rows, w_down, down1)
        snd_f, acts = barrier((snd_f, acts))
        sum_f = (own_f + core_swap(snd_f).astype(F32)).astype(BF16)
        sum_f_y = y_swap(sum_f)
        caches = write(4, acts, caches)
        sum_f_y, caches = barrier((sum_f_y, caches))
        moe_m = sum_m.astype(F32) + sum_m_y.astype(F32)
        moe_f = sum_f.astype(F32) + sum_f_y.astype(F32)
        moe = jnp.where(cx == 0, jnp.concatenate([moe_m, moe_f]), jnp.concatenate([moe_f, moe_m]))
        hidden = (x1.astype(F32) + moe).astype(BF16).reshape(steps, batch, width)
        k_new, v_new = caches
        return hidden, back(k_new), back(v_new)

    return jax.shard_map(layer, mesh=mesh, in_specs=in_specs, out_specs=out_specs, check_vma=False)
```

```python
import functools

import jax
import jax.numpy as jnp
from jax import lax
from jax.experimental import pallas as pl
from jax.experimental.pallas import tpu as pltpu
from jax.sharding import PartitionSpec as P


EPS = 1e-5
ROPE_BASE = 1.0e6
F32 = jnp.float32
BF16 = jnp.bfloat16
VMEM_LIMIT = 60 * 1024 * 1024
LANE = 128
WIDE = 256
NB = 8


def cost(flops, moved):
    return pl.CostEstimate(flops=flops, bytes_accessed=moved, transcendentals=0)


def fixed(*shape):
    return pl.BlockSpec(shape, lambda *_: (0,) * len(shape))


def lead(*shape):
    return pl.BlockSpec(shape, lambda i, *_: (i,) + (0,) * (len(shape) - 1))


def norm_into(me, refs, tokens, hs):
    place = [me, me + 1 - 2 * (me % 2), (me + 2) % 4]
    place.append((place[1] + 2) % 4)
    rt = LANE
    width = refs[0].shape[1]
    gains = [r[tokens : tokens + 1, :].astype(F32) for r in refs]

    def body(i, carry):
        rows = pl.ds(pl.multiple_of(i * rt, rt), rt)
        sq = []
        for r in refs:
            v = r[rows, :].astype(F32)
            sq.append(jnp.sum(v * v, axis=-1, keepdims=True))
        total = (sq[0] + sq[1]) + (sq[2] + sq[3])
        scale = lax.rsqrt(total / (4.0 * refs[0].shape[1]) + EPS)
        for n, r in enumerate(refs):
            hs[rows, pl.ds(pl.multiple_of(place[n] * width, LANE), width)] = (r[rows, :].astype(F32) * scale * gains[n]).astype(BF16)
        return carry

    lax.fori_loop(0, tokens // rt, body, 0)


def project(me, hs, refs, ws, cos_ref, sin_ref, out_ref, turn):
    place = [me, me + 1 - 2 * (me % 2), (me + 2) % 4]
    place.append((place[1] + 2) % 4)
    for n, ref in enumerate(refs):
        ws[pl.ds(pl.multiple_of(place[n] * ref.shape[1], LANE), ref.shape[1]), :] = ref[0]
    low = lax.broadcasted_iota(jnp.int32, (1, WIDE), 1) % 64 < 32
    mt = hs.shape[0]
    for m in range(hs.shape[0] // mt):
        rows = slice(m * mt, (m + 1) * mt)
        acc = jnp.dot(hs[rows, :], ws[...], preferred_element_type=F32)
        v = acc.astype(BF16).astype(F32)
        other = jnp.where(low, pltpu.roll(v, 224, 1), pltpu.roll(v, 32, 1))
        cos, sin = cos_ref[rows, :], sin_ref[rows, :]
        if turn is not None:
            cos, sin = jnp.where(turn, cos, 1.0), jnp.where(turn, sin, 0.0)
        cos = jnp.concatenate([cos] * 2, axis=1)
        sin = jnp.concatenate([sin] * 2, axis=1)
        out_ref[0, rows, :] = (v * cos + other * sin).astype(BF16)


def qkv_a_kernel(me_ref, x0, x1, x2, x3, w0, w1, w2, w3, cos_ref, sin_ref, hs, out_ref, ws):
    @pl.when(pl.program_id(0) == 0)
    def _():
        norm_into(me_ref[0], (x0, x1, x2, x3), cos_ref.shape[0], hs)

    project(me_ref[0], hs, (w0, w1, w2, w3), ws, cos_ref, sin_ref, out_ref, None)


def qkv_b_kernel(me_ref, hs, w0, w1, w2, w3, cos_ref, sin_ref, before, out_ref, ws):
    project(me_ref[0], hs, (w0, w1, w2, w3), ws, cos_ref, sin_ref, out_ref, pl.program_id(0) < 2)


def qkv_calls(me, xs, was, wbs, cos, sin):
    tokens = cos.shape[0]
    rows, width = xs[0].shape
    na, nb = was[0].shape[0], wbs[0].shape[0]
    full = jax.ShapeDtypeStruct((na + nb, tokens, WIDE), BF16)
    w_spec = [lead(1, width, WIDE)] * 4
    t_spec = [fixed(tokens, LANE)] * 2
    h_spec = fixed(tokens, 4 * width)
    params = pltpu.CompilerParams(vmem_limit_bytes=VMEM_LIMIT, dimension_semantics=("arbitrary",))
    h, first = pl.pallas_call(
        qkv_a_kernel,
        grid_spec=pltpu.PrefetchScalarGridSpec(
            num_scalar_prefetch=1,
            grid=(na,),
            in_specs=[fixed(rows, width)] * 4 + w_spec + t_spec,
            out_specs=[h_spec, lead(1, tokens, WIDE)],
            scratch_shapes=[pltpu.VMEM((4 * width, WIDE), BF16)],
        ),
        out_shape=[jax.ShapeDtypeStruct((tokens, 4 * width), BF16), full],
        compiler_params=params,
        cost_estimate=cost(2 * tokens * width * 4 * 512, 6_000_000),
        name="qkv_a",
    )(me, *xs, *was, cos, sin)
    return pl.pallas_call(
        qkv_b_kernel,
        grid_spec=pltpu.PrefetchScalarGridSpec(
            num_scalar_prefetch=1,
            grid=(nb,),
            in_specs=[h_spec] + w_spec + t_spec + [pl.BlockSpec(memory_space=pl.ANY)],
            out_specs=pl.BlockSpec((1, tokens, WIDE), lambda i, m: (na + i, 0, 0)),
            scratch_shapes=[pltpu.VMEM((4 * width, WIDE), BF16)],
        ),
        out_shape=full,
        input_output_aliases={8: 0},
        compiler_params=params,
        cost_estimate=cost(2 * tokens * width * 4 * 768, 6_000_000),
        name="qkv_b",
    )(me, h, *wbs, cos, sin, first)


def by_sequence(a_ref, rows_ref, turned_ref):
    kinds, count, _ = a_ref.shape
    for side in range(2):
        lanes = slice(side * LANE, side * LANE + LANE)
        for r in range(kinds):
            rows_ref[side, r * count : (r + 1) * count, :] = a_ref[r, :, lanes].astype(F32)
        rows_ref[side, kinds * count :, :] = jnp.zeros((count, LANE), F32)
        for i in range(count):
            turned_ref[i * 16 : i * 16 + 16, lanes] = rows_ref[side, pl.ds(i, 16, stride=count), :].astype(turned_ref.dtype)


def attn_kernel(off_ref, len_ref, a_ref, k_ref, k2_ref, v_ref, v2_ref, o_ref, lhs_ref, snew_ref, enew_ref, rows_ref, turned_ref):
    base = (off_ref[0] + pl.program_id(0)) * NB
    slot = lax.broadcasted_iota(jnp.int32, (1, WIDE), 1)
    block = slot // 64
    row = lax.broadcasted_iota(jnp.int32, (64, LANE), 0) % 16 % 3
    col = lax.broadcasted_iota(jnp.int32, (64, LANE), 1)
    by_sequence(a_ref, rows_ref, turned_ref)
    every = turned_ref[...]
    scaled = every * jnp.bfloat16(0.125)
    for i in range(NB):
        q = scaled[i * 16 : i * 16 + 16]
        zero = jnp.zeros_like(q)
        lhs_ref[i * 64 : i * 64 + 64, :] = jnp.concatenate([jnp.where(block == k, q, zero) for k in range(4)], axis=0)
    snew_ref[...] = lax.dot_general(lhs_ref[...], every, (((1,), (1,)), ((), ())), preferred_element_type=F32)
    totals, mixes = [], []
    for i in range(NB):
        pos = len_ref[base + i]
        rows = slice(i * 64, i * 64 + 64)
        s_old = jnp.dot(lhs_ref[rows, :], (k_ref, k2_ref)[i // 4][i % 4 * WIDE : (i % 4 + 1) * WIDE, :], preferred_element_type=F32)
        fresh = (col >= i * 16 + 9) & (col <= row + (i * 16 + 9))
        s_old = jnp.where(slot < pos, s_old, -1.0e30)
        s_new = jnp.where(fresh, snew_ref[rows, :], -1.0e30)
        peak = jnp.max(jnp.maximum(jnp.maximum(s_old[:, :LANE], s_old[:, LANE:]), s_new), axis=-1, keepdims=True)
        e_old = jnp.exp(s_old - peak)
        e_new = jnp.exp(s_new - peak)
        enew_ref[rows, :] = e_new.astype(BF16)
        total = jnp.sum(e_old[:, :LANE] + e_old[:, LANE:] + e_new, axis=-1, keepdims=True)
        mixed = lax.dot_general(e_old.astype(BF16), (v_ref, v2_ref)[i // 4][i % 4 * WIDE : (i % 4 + 1) * WIDE, :], (((1,), (1,)), ((), ())), preferred_element_type=F32)
        res = mixed[0:16]
        tot = jnp.broadcast_to(total[0:16], (16, WIDE))
        for k in range(1, 4):
            part = slice(16 * k, 16 * k + 16)
            res = jnp.where(block == k, mixed[part], res)
            tot = jnp.where(block == k, total[part], tot)
        mixes.append(res)
        totals.append(tot)
    fresh_v = jnp.concatenate([every[3:], every[:3]], axis=0)
    extra = jnp.dot(enew_ref[...], fresh_v, preferred_element_type=F32)
    for i in range(NB):
        res = extra[i * 64 : i * 64 + 16]
        for k in range(1, 4):
            res = jnp.where(block == k, extra[i * 64 + 16 * k : i * 64 + 16 * k + 16], res)
        o_ref[i] = ((mixes[i] + res) / totals[i]).astype(BF16)


def attn_call(offset, lengths, acts, k_rows, v_rows, count):
    even = pl.BlockSpec((NB * LANE, WIDE), lambda i, f, m: (2 * (f[0] + i), 0))
    odd = pl.BlockSpec((NB * LANE, WIDE), lambda i, f, m: (2 * (f[0] + i) + 1, 0))
    grid_spec = pltpu.PrefetchScalarGridSpec(
        num_scalar_prefetch=2,
        grid=(count // NB,),
        in_specs=[pl.BlockSpec((15, NB, WIDE), lambda i, f, m: (0, f[0] + i, 0)), even, odd, even, odd],
        out_specs=lead(NB, 16, WIDE),
        scratch_shapes=[pltpu.VMEM((NB * 64, WIDE), BF16), pltpu.VMEM((NB * 64, LANE), F32), pltpu.VMEM((NB * 64, LANE), BF16), pltpu.VMEM((2, NB * 16, LANE), F32), pltpu.VMEM((NB * 16, WIDE), BF16)],
    )
    return pl.pallas_call(
        attn_kernel,
        grid_spec=grid_spec,
        out_shape=jax.ShapeDtypeStruct((count, 16, WIDE), BF16),
        compiler_params=pltpu.CompilerParams(vmem_limit_bytes=VMEM_LIMIT, dimension_semantics=("arbitrary",)),
        cost_estimate=cost(count * 120_000_000, count * 262144),
        name="attn",
    )(offset, lengths, acts, k_rows, k_rows, v_rows, v_rows)


WB = 16
PIECES = (32, 64, 96, 32, 32)


def write_kernel(start, aliased, len_ref, a_ref, k_ref, v_ref, *rest):
    ko_ref, vo_ref, rows_ref, turned_ref = rest[2:] if aliased else rest
    by_sequence(a_ref, rows_ref, turned_ref)
    base = start + pl.program_id(0) * WB
    cols = jnp.transpose(turned_ref[...])
    slot = lax.broadcasted_iota(jnp.int32, (1, WIDE), 1)
    for i in range(WB):
        pos = len_ref[base + i]
        rows = slice(i * WIDE, (i + 1) * WIDE)
        hit = (slot >= pos) & (slot <= pos + 2)
        part = cols[:, (i // 8) * LANE : (i // 8) * LANE + LANE]
        for first, src, dst in ((9, k_ref, ko_ref), (12, v_ref, vo_ref)):
            moved = pltpu.roll(part, (pos - (i % 8) * 16 - first + WIDE) % LANE, 1).astype(BF16)
            for side in range(2):
                lanes = slice(side * LANE, side * LANE + LANE)
                dst[rows, lanes] = jnp.where(hit[:, lanes], moved, src[rows, lanes])


def write_call(start, count, lengths, acts, k_rows, v_rows, before):
    s0 = start // WB
    block = pl.BlockSpec((WB * WIDE, WIDE), lambda i, m: (s0 + i, 0))
    aliased = before is not None
    grid_spec = pltpu.PrefetchScalarGridSpec(
        num_scalar_prefetch=1,
        grid=(count // WB,),
        in_specs=[pl.BlockSpec((15, WB, WIDE), lambda i, m: (0, s0 + i, 0)), block, block]
        + ([pl.BlockSpec(memory_space=pl.ANY)] * 2 if aliased else []),
        out_specs=[block, block],
        scratch_shapes=[pltpu.VMEM((2, WB * 16, LANE), F32), pltpu.VMEM((WB * 16, WIDE), F32)],
    )
    return pl.pallas_call(
        functools.partial(write_kernel, start, aliased),
        grid_spec=grid_spec,
        out_shape=[jax.ShapeDtypeStruct(k_rows.shape, BF16)] * 2,
        input_output_aliases={4: 0, 5: 1} if aliased else {},
        compiler_params=pltpu.CompilerParams(vmem_limit_bytes=VMEM_LIMIT, dimension_semantics=("arbitrary",)),
        cost_estimate=cost(count * 180_000_000, count * 524288),
        name="write",
    )(lengths, acts, k_rows, v_rows, *(before if aliased else ()))


E1 = 8


def moe1_kernel(half_ref, h_ref, ch_ref, a0, l0, a1, l1, out_ref, dense):
    step = pl.program_id(0)
    half = out_ref.shape[1]
    rt = 16

    @pl.when(step == 0)
    def _():
        out_ref[...] = jnp.zeros_like(out_ref)

    for g in range(E1 // 4):
        for k in range(4):
            e = g * 4 + k
            top = jnp.concatenate([a0[e], l0[e]], axis=1)
            low = jnp.concatenate([a1[e], l1[e]], axis=1)
            w = jnp.concatenate([top, low], axis=0)
            dense[g, k] = jnp.dot(h_ref[...], w, preferred_element_type=F32).astype(BF16)
        ids = [(step * E1 + g * 4 + k).astype(F32).astype(BF16) for k in range(4)]
        for i in range(half // rt):
            rows = slice(i * rt, (i + 1) * rt)
            d = [dense[g, k, rows, :] for k in range(4)]
            for j in range(8):
                chj = ch_ref[j, rows, :]
                hits = [chj == ids[k] for k in range(4)]
                for side in range(2):
                    lanes = slice(side * LANE, side * LANE + LANE)
                    acc = out_ref[j, rows, lanes]
                    for k in range(4):
                        acc = jnp.where(hits[k], d[k][:, lanes], acc)
                    out_ref[j, rows, lanes] = acc


def moe1_call(pick, h2, ch, w_act, w_lin, a1, l1):
    half = h2.shape[0] // 2
    experts, rows, _ = a1.shape
    mine = pl.BlockSpec((E1, rows, LANE), lambda i, m: (i, 0, m[1]))
    theirs = lead(E1, rows, LANE)
    grid_spec = pltpu.PrefetchScalarGridSpec(
        num_scalar_prefetch=1,
        grid=(experts // E1,),
        in_specs=[pl.BlockSpec((half, 2 * rows), lambda i, m: (m[0], 0)), pl.BlockSpec((8, half, LANE), lambda i, m: (0, m[0], 0)), mine, mine, theirs, theirs],
        out_specs=fixed(8, half, WIDE),
        scratch_shapes=[pltpu.VMEM((E1 // 4, 4, half, WIDE), BF16)],
    )
    return pl.pallas_call(
        moe1_kernel,
        grid_spec=grid_spec,
        out_shape=jax.ShapeDtypeStruct((8, half, WIDE), BF16),
        compiler_params=pltpu.CompilerParams(vmem_limit_bytes=VMEM_LIMIT, dimension_semantics=("arbitrary",)),
        cost_estimate=cost(2 * half * 2 * rows * WIDE * experts, 20_000_000),
        name="moe1",
    )(pick, h2, ch, w_act, w_lin, a1, l1)


E2 = 8


def moe2_kernel(half_ref, u_ref, ch_ref, wa, wb, own_ref, send_ref, spread, acc_ref):
    step = pl.program_id(0)
    half = u_ref.shape[1]
    width = wa.shape[2]
    rt = 16

    @pl.when(step == 0)
    def _():
        acc_ref[...] = jnp.zeros_like(acc_ref)

    prod = None
    for g in range(E2 // 4):
        ids = [(step * E2 + g * 4 + k).astype(F32).astype(BF16) for k in range(4)]
        for i in range(half // rt):
            rows = slice(i * rt, (i + 1) * rt)
            out = [jnp.zeros((rt, LANE), BF16) for _ in range(4)]
            for j in range(8):
                chj = ch_ref[j, rows, :]
                uj = u_ref[j, rows, :]
                for k in range(4):
                    out[k] = jnp.where(chj == ids[k], uj, out[k])
            for k in range(4):
                spread[g, rows, k * LANE : (k + 1) * LANE] = out[k]
        es = slice(g * 4, g * 4 + 4)
        w = jnp.concatenate([wa[es].reshape(512, width), wb[es].reshape(512, width)], axis=1)
        part = jnp.dot(spread[g], w, preferred_element_type=F32)
        prod = part if prod is None else prod + part
    acc_ref[...] += prod

    @pl.when(step == pl.num_programs(0) - 1)
    def _():
        own_ref[...] = acc_ref[:, :width]
        send_ref[...] = acc_ref[:, width:].astype(BF16)


def moe2_call(pick, u, ch, w_down, wb):
    half = u.shape[1]
    experts, rows, width = wb.shape
    grid_spec = pltpu.PrefetchScalarGridSpec(
        num_scalar_prefetch=1,
        grid=(experts // E2,),
        in_specs=[
            fixed(8, half, LANE),
            pl.BlockSpec((8, half, LANE), lambda i, m: (0, m[0], 0)),
            pl.BlockSpec((E2, rows, width), lambda i, m: (i, m[1], 0)),
            lead(E2, rows, width),
        ],
        out_specs=[fixed(half, width)] * 2,
        scratch_shapes=[pltpu.VMEM((E2 // 4, half, 512), BF16), pltpu.VMEM((half, 2 * width), F32)],
    )
    return pl.pallas_call(
        moe2_kernel,
        grid_spec=grid_spec,
        out_shape=[jax.ShapeDtypeStruct((half, width), F32), jax.ShapeDtypeStruct((half, width), BF16)],
        compiler_params=pltpu.CompilerParams(vmem_limit_bytes=VMEM_LIMIT, dimension_semantics=("arbitrary",)),
        cost_estimate=cost(2 * half * rows * 2 * width * experts, 10_000_000),
        name="moe2",
    )(pick, u, ch, w_down, wb)


def solution(mesh):
    cache_spec = P('dp', None, 'y', None)
    in_specs = (P(None, 'dp'), P('dp'), P(None, 'dp', None), P(None, 'x'), cache_spec, cache_spec, P('x'), P('x', 'y'), P('x', 'y'), P('x', 'y'), P('y', 'x'), P('x'), P('x', None), P(None, 'x', 'y'), P(None, 'x', 'y'), P(None, 'y', 'x'))
    out_specs = (P(None, 'dp', 'x'), cache_spec, cache_spec)

    def core_swap(v):
        return lax.ppermute(v, 'x', [(0, 1), (1, 0), (2, 3), (3, 2)])

    def chip_swap(v):
        return lax.ppermute(v, 'x', [(0, 2), (2, 0), (1, 3), (3, 1)])

    def y_swap(v):
        return lax.ppermute(v, 'y', [(0, 1), (1, 0)])

    def layer(tokens, lengths, choices, emb_table, k_cache, v_cache, g_attn, w_q, w_k, w_v, w_o, g_ffn, w_router, w_act, w_lin, w_down):
        steps, batch = tokens.shape
        width = emb_table.shape[1]
        kv, hd = k_cache.shape[2], k_cache.shape[3]
        slots = k_cache.shape[1]
        group = w_q.shape[1] // (kv * hd)
        experts = w_act.shape[0]
        width_full = width * 4
        me = lax.axis_index('x').astype(jnp.int32)
        my = lax.axis_index('y').astype(jnp.int32)
        core = me % 2
        cx = me // 2
        n_tok = steps * batch

        barrier = lax.optimization_barrier
        wq = w_q.reshape(width, kv, group, hd).transpose(2, 0, 1, 3).reshape(group, width, kv * hd)
        w_a = wq[:2]
        w_b = jnp.concatenate([wq[2:], w_k[None], w_v[None]], axis=0)
        half_tok = n_tok // 2
        x_in = jnp.take(emb_table, tokens.reshape(n_tok), axis=0, mode='clip')
        g_rows = jnp.concatenate([g_attn[None], g_ffn[None], jnp.zeros((14, width), BF16)], axis=0)
        x_ext = jnp.concatenate([x_in, g_rows])
        part = jnp.concatenate([lax.dynamic_slice_in_dim(x_in, my * half_tok, half_tok, 0), g_rows], axis=0)
        part, x_ext = barrier((part, x_ext))
        part = chip_swap(part)
        x_mate = core_swap(x_ext)
        wa2 = chip_swap(w_a)
        wb2 = chip_swap(w_b)
        positions = lengths[None, :] + jnp.arange(steps, dtype=jnp.int32)[:, None]
        inv_freq = ROPE_BASE ** (-(jnp.arange(hd // 2, dtype=F32) * 2.0 / hd))
        angles = positions.reshape(n_tok).astype(F32)[:, None] * inv_freq[None, :]
        cos, sin = jnp.cos(angles), jnp.sin(angles)
        cos2, sin2 = jnp.concatenate([cos] * 4, axis=1), jnp.concatenate([-sin, sin] * 2, axis=1)
        choice_rows = choices.reshape(n_tok, 8)
        ch_rows = jnp.broadcast_to(choice_rows.T.astype(BF16)[:, :, None], (8, n_tok, LANE))

        def theirs(w, axis):
            return lax.dynamic_slice_in_dim(w, (1 - core) * LANE, LANE, axis)

        act_s = theirs(w_act, 2)
        lin_s = theirs(w_lin, 2)
        part, act_s = barrier((part, act_s))
        part_o = y_swap(part[:half_tok])
        part_o, lin_s, ch_rows, cos2, sin2 = barrier((part_o, lin_s, ch_rows, cos2, sin2))
        lo = jnp.where(my == 0, part[:half_tok], part_o)
        hi = jnp.where(my == 0, part_o, part[:half_tok])
        x_far = jnp.concatenate([lo, hi, part[half_tok:]])
        x_far_mate = core_swap(x_far)
        wa1, wb1, wa3 = core_swap(w_a), core_swap(w_b), core_swap(wa2)

        router = jnp.concatenate([w_router, core_swap(w_router)], axis=0)


        pick_m, pick_f = jnp.stack([cx, core]), jnp.stack([1 - cx, core])
        offset = (me * (batch // 4) // NB)[None]
        wb3 = core_swap(wb2)
        act1, lin1 = core_swap(act_s), core_swap(lin_s)
        qkv = qkv_calls(me[None], (x_ext, x_mate, x_far, x_far_mate), (w_a, wa1, wa2, wa3), (w_b, wb1, wb2, wb3), cos2, sin2)
        acts = qkv.reshape(5 * steps, batch, WIDE)
        k_rows = k_cache.transpose(0, 2, 3, 1).reshape(batch * kv * hd, slots)
        v_rows = v_cache.transpose(0, 2, 3, 1).reshape(batch * kv * hd, slots)
        starts = [sum(PIECES[:i]) for i in range(len(PIECES))]

        def write(i, acts, before):
            return tuple(write_call(starts[i], PIECES[i], lengths, acts, k_rows, v_rows, before))

        def back(rows):
            return rows.reshape(batch, kv, hd, slots).transpose(0, 3, 1, 2)

        o = attn_call(offset, lengths, acts, k_rows, v_rows, batch // 4)[:, : steps * group]
        o, acts, w_down, w_o = barrier((o, acts, w_down, w_o))
        wo = w_o.reshape(kv, group, hd, width).transpose(1, 0, 2, 3).reshape(group * kv * hd, width)
        o_far = chip_swap(o)
        down_s = theirs(w_down, 1)
        caches = write(0, acts, None)
        o_far, caches, down_s, wo, pick_m, pick_f = barrier((o_far, caches, down_s, wo, pick_m, pick_f))
        down1 = core_swap(down_s)

        def in_order(v, mate):
            return jnp.where(core == 0, jnp.concatenate([v, mate]), jnp.concatenate([mate, v]))

        near, far = in_order(o, core_swap(o)), in_order(o_far, core_swap(o_far))
        o = jnp.where(cx == 0, jnp.concatenate([near, far]), jnp.concatenate([far, near]))
        oc = o.reshape(batch, group, steps, WIDE).transpose(2, 0, 1, 3).reshape(n_tok, group * WIDE)
        proj = jnp.dot(oc, wo, preferred_element_type=F32).astype(BF16)

        proj, acts = barrier((proj, acts))
        proj_y = y_swap(proj)
        caches = write(1, acts, caches)
        proj_y, caches = barrier((proj_y, caches))

        x1 = (x_in.astype(F32) + (proj.astype(F32) + proj_y.astype(F32))).astype(BF16)
        x1_mate = core_swap(x1)
        x1f, x1mf = x1.astype(F32), x1_mate.astype(F32)
        sq = jnp.sum(x1f * x1f, axis=-1) + jnp.sum(x1mf * x1mf, axis=-1)
        sq = sq + chip_swap(sq)
        scale = lax.rsqrt(sq / width_full + EPS)[:, None]
        g_own, g_mate = g_ffn.astype(F32), x_mate[n_tok + 1].astype(F32)
        h2 = jnp.concatenate([x1f * scale * g_own, x1mf * scale * g_mate], axis=1).astype(BF16)
        logits = jnp.dot(h2, router, preferred_element_type=F32)

        logits_far = chip_swap(logits)
        send = moe1_call(pick_f, h2, ch_rows, w_act, w_lin, act1, lin1)
        send, h2, acts = barrier((send, h2, acts))
        got = chip_swap(send)
        keep = moe1_call(pick_m, h2, ch_rows, w_act, w_lin, act1, lin1)
        caches = write(2, acts, caches)
        logits = logits + logits_far
        picked = jnp.sum(jnp.where(choice_rows[:, :, None] == jnp.arange(experts)[None, None, :], logits[:, None, :], 0.0), axis=-1)
        gate = jax.nn.softmax(picked, axis=-1)
        gate_mine = lax.dynamic_slice_in_dim(gate, cx * half_tok, half_tok, 0).T
        got, caches, gate_mine = barrier((got, caches, gate_mine))
        hid = keep.astype(F32) + got.astype(F32)
        u = (gate_mine[:, :, None] * jax.nn.silu(hid[..., :LANE]) * hid[..., LANE:]).astype(BF16)

        u, acts = barrier((u, acts))
        u_far = chip_swap(u)
        own_m, snd_m = moe2_call(pick_m, u, ch_rows, w_down, down1)
        caches = write(3, acts, caches)
        sum_m = (own_m + core_swap(snd_m).astype(F32)).astype(BF16)
        u_far, caches, acts, sum_m = barrier((u_far, caches, acts, sum_m))
        sum_m_y = y_swap(sum_m)
        own_f, snd_f = moe2_call(pick_f, u_far, ch_rows, w_down, down1)
        snd_f, acts = barrier((snd_f, acts))
        sum_f = (own_f + core_swap(snd_f).astype(F32)).astype(BF16)
        sum_f_y = y_swap(sum_f)
        caches = write(4, acts, caches)
        sum_f_y, caches = barrier((sum_f_y, caches))
        moe_m = sum_m.astype(F32) + sum_m_y.astype(F32)
        moe_f = sum_f.astype(F32) + sum_f_y.astype(F32)
        moe = jnp.where(cx == 0, jnp.concatenate([moe_m, moe_f]), jnp.concatenate([moe_f, moe_m]))
        hidden = (x1.astype(F32) + moe).astype(BF16).reshape(steps, batch, width)
        k_new, v_new = caches
        return hidden, back(k_new), back(v_new)

    return jax.shard_map(layer, mesh=mesh, in_specs=in_specs, out_specs=out_specs, check_vma=False)
```
